32 devices in a mesh: data: 1 (over z), row: 4 (over y), col: 4 (over x), core: 2 (over core).
Axes of the slice: x: 4, y: 4, z: 1, core: 2. Of those that a mesh axis runs over, the one named last changes fastest.
The devices are a block of a 4x4x8 slice.
Arguments:
- tokens: bfloat16 [2, 2048, 2048], P('data', ('row', 'col', 'core'))
- w_qkv: bfloat16 [2048, 3, 32, 64], replicated
- w_out: bfloat16 [32, 64, 2048], replicated
Outputs:
- output: bfloat16 [2, 2048, 2048], P('data', ('row', 'col', 'core'))
All inputs are finite; a program needn't handle non-finite values.
Results may differ from the reference program's by a relative error of at most 0.00748467.
Values are sent between devices in bfloat16 or wider.
A program may use at most 768 MiB of HBM per device.

```python
import jax
import jax.numpy as jnp
from jax import lax

SEQ = 2048
HEADS = 32
HEAD = 64
BATCH = 2
QUERY_BLOCK = 64

CH = HEADS * HEAD


def setup_inputs(seed: int = 0, part: int = 0) -> dict:
    base_key = jax.random.key(seed)
    tok_key = jax.random.fold_in(jax.random.fold_in(base_key, 1), part)
    qkv_key, out_key = jax.random.split(jax.random.fold_in(base_key, 2))
    tokens = jax.random.normal(tok_key, (BATCH, SEQ, CH), jnp.float32)
    w_qkv = jax.random.normal(qkv_key, (CH, 3, HEADS, HEAD), jnp.float32) * (1.5 * CH ** -0.5)
    out_gain = (SEQ / 160.0) ** 0.5 / 1.5
    w_out = jax.random.normal(out_key, (HEADS, HEAD, CH), jnp.float32) * (out_gain * CH ** -0.5)
    return {"tokens": tokens.astype(jnp.bfloat16), "w_qkv": w_qkv.astype(jnp.bfloat16), "w_out": w_out.astype(jnp.bfloat16)}


def reference(tokens, w_qkv, w_out):
    flat_rows = tokens.reshape(BATCH * SEQ, CH)
    qkv_all = jnp.dot(flat_rows, w_qkv.reshape(CH, 3 * CH), preferred_element_type=jnp.float32).astype(jnp.bfloat16)
    qkv_all = qkv_all.astype(jnp.float32).reshape(BATCH, SEQ, 3, HEADS, HEAD)
    per_head = jnp.transpose(qkv_all, (3, 2, 0, 1, 4))
    logit_scale = HEAD ** -0.5
    num_qblk = SEQ // QUERY_BLOCK

    def one_head(head_qkv):
        queries = head_qkv[0].reshape(BATCH, num_qblk, QUERY_BLOCK, HEAD).transpose(1, 0, 2, 3)
        key_rows = head_qkv[1]
        value_rows = head_qkv[2]

        def one_block(q_blk):
            scores = jnp.einsum("bqd,bkd->bqk", q_blk, key_rows) * logit_scale
            attn_prob = jax.nn.softmax(scores, axis=-1)
            return jnp.einsum("bqk,bkd->bqd", attn_prob, value_rows)

        out_blk = lax.map(one_block, queries)
        return out_blk.transpose(1, 0, 2, 3).reshape(BATCH, SEQ, HEAD)

    heads_out = lax.map(one_head, per_head)
    attn_rows = jnp.transpose(heads_out, (1, 2, 0, 3)).reshape(BATCH * SEQ, CH).astype(jnp.bfloat16)
    y_rows = jnp.dot(attn_rows, w_out.reshape(CH, CH), preferred_element_type=jnp.float32).astype(jnp.bfloat16)
    return y_rows.reshape(BATCH, SEQ, CH)
```

```python
import functools

import jax
import jax.numpy as jnp
from jax import lax
from jax.experimental import pallas as pl
from jax.experimental.pallas import tpu as pltpu
from jax.sharding import PartitionSpec as P

MESH = pl.DeviceIdType.MESH
F32 = jnp.float32
BF16 = jnp.bfloat16
NT = (((1,), (1,)), ((), ()))
NN = (((1,), (0,)), ((), ()))


def hop_order(rows, cols):
    def hops(d, n):
        return min(d, n - d)

    offs = [(dy, dx) for dy in range(rows) for dx in range(cols)][1:]
    return sorted(offs, key=lambda o: (-hops(o[0], rows) - hops(o[1], cols), hops(o[0], rows), hops(o[1], cols)))


def pack_table(values, base):
    words = []
    for start in range(0, len(values), 8):
        words.append(sum(v * base**i for i, v in enumerate(values[start : start + 8])))
    return words


def kernel(dims, x_ref, wt_ref, wo_ref, y_ref, wbuf, wobuf, sbuf, kv_all, q_all, vt, s0, s1, obuf, ob,
           w_sem, wo_sem, send_sem, recv_sem, osend_sem, orecv_sem):
    rows, cols, tok, pair, head = dims
    chips = rows * cols
    ch = x_ref.shape[1]
    z = lax.axis_index("data")
    r = lax.axis_index("row")
    c = lax.axis_index("col")
    k = lax.axis_index("core")
    my_chip = r * cols + c
    me = my_chip * 2 + k
    order = hop_order(rows, cols)
    n_step = len(order)
    dy_words = pack_table([o[0] for o in order], rows)
    dx_words = pack_table([o[1] for o in order], cols)

    def digit(words, base, i):
        val = words[0]
        for w, word in enumerate(words[1:]):
            val = val + (word - words[w]) * (jnp.minimum(i // (8 * (w + 1)), 1))
        shift = base.bit_length() - 1
        return lax.rem(lax.shift_right_logical(jnp.int32(0) + val, shift * lax.rem(i, 8)), base)

    def step_offset(i):
        if isinstance(i, int):
            return order[i]
        return digit(dy_words, rows, i), digit(dx_words, cols, i)

    def chip_to(i):
        dy, dx = step_offset(i)
        rr, cc = lax.rem(r + dy, rows), lax.rem(c + dx, cols)
        return rr, cc, rr * cols + cc

    def chip_from(i):
        dy, dx = step_offset(i)
        rr, cc = lax.rem(r + rows - dy, rows), lax.rem(c + cols - dx, cols)
        return rr, cc, rr * cols + cc

    def w_copy(slot, j, chip):
        return pltpu.make_async_copy(
            wt_ref.at[pl.ds(pl.multiple_of((j * chips + chip) * pair, pair), pair)],
            wbuf.at[slot, j], w_sem.at[j, slot])

    for j in (1, 2, 0):
        w_copy(0, j, my_chip).start()
    for i in range(n_step):
        chip = chip_to(i)[2]
        w_copy(i + 1, 1, chip).start()
        w_copy(i + 1, 2, chip).start()

    barrier = pltpu.get_barrier_semaphore()
    for i in range(n_step):
        rr, cc, _ = chip_to(i)
        for core in range(2):
            pl.semaphore_signal(barrier, inc=1, device_id=(z, rr, cc, core), device_id_type=MESH)
    pl.semaphore_signal(barrier, inc=1, device_id=(z, r, c, 1 - k), device_id_type=MESH)
    for i in range(n_step):
        w_copy(i + 1, 0, chip_to(i)[2]).start()
    wo_copy = pltpu.make_async_copy(wo_ref, wobuf, wo_sem)
    wo_copy.start()

    def project(slot, j):
        return lax.dot_general(x_ref[...], wbuf[slot, j], NT, preferred_element_type=F32).astype(BF16)

    def keep(slot, j, piece):
        val = project(slot, j)
        for b in range(2):
            sbuf[slot, b, piece] = val[b * tok:(b + 1) * tok]

    def kv_send(slot, b, rr, cc):
        return pltpu.make_async_remote_copy(
            src_ref=sbuf.at[slot, b, pl.ds(0, 2)], dst_ref=kv_all.at[:, me],
            send_sem=send_sem.at[0, slot, b], recv_sem=recv_sem.at[0, me],
            device_id=(z, rr, cc, b), device_id_type=MESH)

    def q_send(slot, b, rr, cc):
        return pltpu.make_async_remote_copy(
            src_ref=sbuf.at[slot, b, 2], dst_ref=q_all.at[me],
            send_sem=send_sem.at[1, slot, b], recv_sem=recv_sem.at[1, me],
            device_id=(z, rr, cc, b), device_id_type=MESH)

    def kv_wait(dev):
        pltpu.make_async_remote_copy(
            src_ref=sbuf.at[0, 0, pl.ds(0, 2)], dst_ref=kv_all.at[:, dev],
            send_sem=send_sem.at[0, 0, 0], recv_sem=recv_sem.at[0, dev],
            device_id=(z, r, c, k), device_id_type=MESH).wait_recv()

    def q_wait(dev):
        pltpu.make_async_remote_copy(
            src_ref=sbuf.at[0, 0, 2], dst_ref=q_all.at[dev],
            send_sem=send_sem.at[1, 0, 0], recv_sem=recv_sem.at[1, dev],
            device_id=(z, r, c, k), device_id_type=MESH).wait_recv()

    for j, piece in ((1, 0), (2, 1), (0, 2)):
        w_copy(0, j, my_chip).wait()
        keep(0, j, piece)
    for piece in range(2):
        kv_all[piece, me] = sbuf[0, k, piece]
    q_all[me] = sbuf[0, k, 2]

    pl.semaphore_wait(barrier, 2 * n_step + 1)
    kv_send(0, 1 - k, r, c).start()
    q_send(0, 1 - k, r, c).start()

    def kv_step(i, _):
        rr, cc, chip = chip_to(i)
        for j, piece in ((1, 0), (2, 1)):
            w_copy(i + 1, j, chip).wait()
            keep(i + 1, j, piece)
        for b in range(2):
            kv_send(i + 1, b, rr, cc).start()
        return 0

    def q_step(i, _):
        rr, cc, chip = chip_to(i)
        w_copy(i + 1, 0, chip).wait()
        keep(i + 1, 0, 2)
        for b in range(2):
            q_send(i + 1, b, rr, cc).start()
        return 0

    lax.fori_loop(0, n_step, kv_step, 0)
    lax.fori_loop(0, n_step, q_step, 0)

    def flip(chip):
        val = kv_all[1, pl.ds(2 * chip, 2)].reshape(2 * tok, pair)
        vt[:, pl.ds(pl.multiple_of(chip * 2 * tok, 2 * tok), 2 * tok)] = val.T

    def kv_arrive(i, _):
        _, _, chip = chip_from(i)
        kv_wait(2 * chip)
        kv_wait(2 * chip + 1)
        flip(chip)
        return 0

    lax.fori_loop(0, n_step, kv_arrive, 0)
    kv_wait(2 * my_chip + 1 - k)
    flip(my_chip)

    keys = kv_all.shape[1] * tok
    chunk = 4 * 2 * tok
    n_chunk = keys // chunk
    lanes = 2 * 2 * tok

    def queries(chip):
        q = q_all[pl.ds(2 * chip, 2)].reshape(2 * tok, pair) * BF16(head**-0.5)
        lane = lax.broadcasted_iota(jnp.int32, q.shape, 1)
        first = lane < head
        zero = jnp.zeros_like(q)
        return jnp.concatenate([jnp.where(first, q, zero), jnp.where(first, zero, q)], axis=0)

    def scores(qq, scr, ci):
        keys_c = kv_all[0, pl.ds(ci * (chunk // tok), chunk // tok)].reshape(chunk, pair)
        s = lax.dot_general(keys_c, qq, NT, preferred_element_type=F32)
        scr[pl.ds(ci * chunk, chunk)] = s
        return jnp.max(s.reshape(chunk // 8, 8, lanes), axis=0)

    def all_scores(chip, scr):
        qq = queries(chip)
        top = scores(qq, scr, 0)
        for ci in range(1, n_chunk):
            top = jnp.maximum(top, scores(qq, scr, ci))
        return jnp.max(top, axis=0, keepdims=True)

    def finish(chip, scr, top):
        total = jnp.zeros((8, lanes), F32)
        acc = jnp.zeros((pair, lanes), F32)
        for ci in range(n_chunk):
            w = jnp.exp(scr[pl.ds(ci * chunk, chunk)] - top)
            total += jnp.sum(w.reshape(chunk // 8, 8, lanes), axis=0)
            acc += lax.dot_general(vt[:, ci * chunk:(ci + 1) * chunk], w.astype(BF16), NN, preferred_element_type=F32)
        total = jnp.sum(total, axis=0, keepdims=True)
        half = lanes // 2
        out = jnp.concatenate([acc[:head, :half] / total[:, :half], acc[head:, half:] / total[:, half:]], axis=0)
        return out.T.astype(BF16)

    def o_send(slot, core, rr, cc):
        return pltpu.make_async_remote_copy(
            src_ref=obuf.at[slot, core],
            dst_ref=ob.at[k, :, pl.ds(pl.multiple_of(my_chip * pair, pair), pair)],
            send_sem=osend_sem.at[slot, core], recv_sem=orecv_sem.at[me],
            device_id=(z, rr, cc, core), device_id_type=MESH)

    def o_wait(chip, b):
        pltpu.make_async_remote_copy(
            src_ref=obuf.at[0, 0],
            dst_ref=ob.at[b, :, pl.ds(pl.multiple_of(chip * pair, pair), pair)],
            send_sem=osend_sem.at[0, 0], recv_sem=orecv_sem.at[2 * chip + b],
            device_id=(z, r, c, k), device_id_type=MESH).wait_recv()

    def attend(i, _):
        rr, cc, chip = chip_from(i)
        q_wait(2 * chip)
        q_wait(2 * chip + 1)
        top = all_scores(chip, s0)
        out = finish(chip, s0, top)
        for core in range(2):
            obuf[i + 1, core] = out[core * tok:(core + 1) * tok]
            o_send(i + 1, core, rr, cc).start()
        return 0

    lax.fori_loop(0, n_step, attend, 0)
    q_wait(2 * my_chip + 1 - k)
    out = finish(my_chip, s0, all_scores(my_chip, s0))
    for core in range(2):
        obuf[0, core] = out[core * tok:(core + 1) * tok]
    o_send(0, 1 - k, r, c).start()
    ob[k, :, pl.ds(pl.multiple_of(my_chip * pair, pair), pair)] = obuf[0, k]

    wo_copy.wait()

    def o_arrive(i, _):
        _, _, chip = chip_to(i)
        o_wait(chip, 0)
        o_wait(chip, 1)
        return 0

    lax.fori_loop(0, n_step, o_arrive, 0)
    o_wait(my_chip, 1 - k)

    blk = 512

    def out_step(n, _):
        cs = pl.ds(pl.multiple_of(n * blk, blk), blk)
        y = lax.dot_general(ob[...].reshape(2 * tok, ch), wobuf[:, cs], NN, preferred_element_type=F32)
        y_ref[:, cs] = y.astype(BF16)
        return 0

    lax.fori_loop(0, ch // blk, out_step, 0)

    def drain(i, _):
        rr, cc, _ = chip_to(i)
        fr, fc, _ = chip_from(i)
        for b in range(2):
            kv_send(i + 1, b, rr, cc).wait_send()
            q_send(i + 1, b, rr, cc).wait_send()
            o_send(i + 1, b, fr, fc).wait_send()
        return 0

    lax.fori_loop(0, n_step, drain, 0)
    kv_send(0, 1 - k, r, c).wait_send()
    q_send(0, 1 - k, r, c).wait_send()
    o_send(0, 1 - k, r, c).wait_send()


def solution(mesh):
    tok_spec = P("data", ("row", "col", "core"), None)
    rows, cols, cores = mesh.shape["row"], mesh.shape["col"], mesh.shape["core"]

    def per_device(tokens, w_qkv, w_out):
        batch, tok, ch = tokens.shape
        _, _, heads, head = w_qkv.shape
        chips = rows * cols
        pair = heads // chips * head
        dims = (rows, cols, tok, pair, head)
        devs = chips * cores
        keys = devs * tok
        wt = jnp.transpose(w_qkv, (1, 2, 3, 0)).reshape(3 * heads * head, ch)
        wo = w_out.reshape(heads * head, ch)
        dma = pltpu.SemaphoreType.DMA
        y = pl.pallas_call(
            functools.partial(kernel, dims),
            out_shape=jax.ShapeDtypeStruct((batch * tok, ch), BF16),
            in_specs=[
                pl.BlockSpec(memory_space=pltpu.VMEM),
                pl.BlockSpec(memory_space=pl.ANY),
                pl.BlockSpec(memory_space=pl.ANY),
            ],
            out_specs=pl.BlockSpec(memory_space=pltpu.VMEM),
            scratch_shapes=[
                pltpu.VMEM((chips, 3, pair, ch), BF16),
                pltpu.VMEM((heads * head, ch), BF16),
                pltpu.VMEM((chips, 2, 3, tok, pair), BF16),
                pltpu.VMEM((2, devs, tok, pair), BF16),
                pltpu.VMEM((devs, tok, pair), BF16),
                pltpu.VMEM((pair, keys), BF16),
                pltpu.VMEM((keys, 4 * tok), F32),
                pltpu.VMEM((keys, 4 * tok), F32),
                pltpu.VMEM((chips, 2, tok, pair), BF16),
                pltpu.VMEM((2, tok, heads * head), BF16),
                dma((3, chips)),
                dma,
                dma((2, chips, 2)),
                dma((2, devs)),
                dma((chips, 2)),
                dma((devs,)),
            ],
            compiler_params=pltpu.CompilerParams(
                collective_id=0, has_side_effects=True, vmem_limit_bytes=60 * 1024 * 1024),
        )(tokens.reshape(batch * tok, ch), wt, wo)
        return y.reshape(batch, tok, ch)

    return jax.shard_map(per_device, mesh=mesh, in_specs=(tok_spec, P(), P()), out_specs=tok_spec, check_vma=False)
```

```python
import functools

import jax
import jax.numpy as jnp
from jax import lax
from jax.experimental import pallas as pl
from jax.experimental.pallas import tpu as pltpu
from jax.sharding import PartitionSpec as P

MESH = pl.DeviceIdType.MESH
F32 = jnp.float32
BF16 = jnp.bfloat16
NT = (((1,), (1,)), ((), ()))
NN = (((1,), (0,)), ((), ()))
KEY_CHUNK = 512
WIDE = 3
UNIT = 2


def groups_of(n_step):
    sizes = [1, WIDE - 1] + [WIDE] * (n_step // WIDE - 1)
    starts = [sum(sizes[:g]) for g in range(len(sizes))]
    return list(zip(starts, sizes))


def hop_order(rows, cols):
    def hops(d, n):
        return min(d, n - d)

    offs = [(dy, dx) for dy in range(rows) for dx in range(cols)][1:]
    like = [[(2, 2)], [(1, 1), (3, 3)], [(2, 1), (2, 3), (0, 2)], [(1, 2), (3, 2), (2, 0)], [(1, 3), (3, 1), (0, 1)]]
    first = [o for group in like for o in group if o in offs]
    rest = [o for o in offs if o not in first]
    return first + sorted(rest, key=lambda o: -hops(o[0], rows) - hops(o[1], cols))


def pack_table(values, base):
    words = []
    for start in range(0, len(values), 8):
        words.append(sum(v * base**i for i, v in enumerate(values[start : start + 8])))
    return words


def kernel(dims, x_hbm, wt_hbm, wo_hbm, y_hbm, x_ref, wbuf, wqbuf, wobuf, sbuf, k_all, v_all, q_all, vt, s0, s1, obuf, ob, y_ref,
           x_sem, w_sem, wq_sem, wo_sem, send_sem, kv_sem, q_sem, o_sem, y_sem):
    rows, cols, tok, pair, head = dims
    chips = rows * cols
    ch = x_ref.shape[1]
    z = lax.axis_index("data")
    r = lax.axis_index("row")
    c = lax.axis_index("col")
    k = lax.axis_index("core")
    my_chip = r * cols + c
    order = hop_order(rows, cols)
    n_step = len(order)
    groups = groups_of(n_step)
    n_group = len(groups)
    own = 0
    dy_words = pack_table([o[0] for o in order], rows)
    dx_words = pack_table([o[1] for o in order], cols)

    def digit(words, base, i):
        val = words[0]
        for w, word in enumerate(words[1:]):
            val = val + (word - words[w]) * (jnp.minimum(i // (8 * (w + 1)), 1))
        shift = base.bit_length() - 1
        return lax.rem(lax.shift_right_logical(jnp.int32(0) + val, shift * lax.rem(i, 8)), base)

    def step_offset(i):
        if isinstance(i, int):
            return order[i]
        return digit(dy_words, rows, i), digit(dx_words, cols, i)

    def chip_to(i):
        dy, dx = step_offset(i)
        return lax.rem(r + dy, rows), lax.rem(c + dx, cols)

    def chip_from(i):
        dy, dx = step_offset(i)
        return lax.rem(r + rows - dy, rows), lax.rem(c + cols - dx, cols)

    x_copy = pltpu.make_async_copy(x_hbm, x_ref, x_sem)
    x_copy.start()

    def kv_weights(slot, chip, sem):
        for n in range(2):
            pltpu.make_async_copy(wt_hbm.at[(n + 1) * chips + chip], wbuf.at[2 * slot + n], sem).start()

    def q_weights(slot, chip, sem):
        pltpu.make_async_copy(wt_hbm.at[chip], wqbuf.at[slot], sem).start()

    def chip_id(i):
        rr, cc = chip_to(i)
        return rr * cols + cc

    n_q = n_step // WIDE

    def load_kv(g):
        start, count = groups[g]
        for i in range(start, start + count):
            kv_weights(i + 1, chip_id(i), w_sem.at[g])

    def load_q(g):
        for n in range(WIDE):
            i = g * WIDE + n
            q_weights(i + 1, chip_id(i), wq_sem.at[g])

    def loaded(ref, slot, count, sem):
        part = ref.at[pl.ds(slot, count)]
        pltpu.make_async_copy(part, part, sem).wait()

    load_kv(0)
    barrier = pltpu.get_barrier_semaphore()
    for i in range(n_step):
        rr, cc = chip_to(i)
        for core in range(2):
            pl.semaphore_signal(barrier, inc=1, device_id=(z, rr, cc, core), device_id_type=MESH)
    pl.semaphore_signal(barrier, inc=1, device_id=(z, r, c, 1 - k), device_id_type=MESH)

    load_kv(1)

    def project(w):
        return lax.dot_general(w, x_ref[...], NT, preferred_element_type=F32).astype(BF16).T

    def keep(val, piece, slot, n):
        for b in range(2):
            sbuf[piece, slot, b] = val[b * tok:(b + 1) * tok, n * pair:(n + 1) * pair]

    def project_kv(slot, count):
        val = project(wbuf[pl.ds(2 * slot, 2 * count)].reshape(2 * count * pair, ch))
        for n in range(2 * count):
            keep(val, n % 2, slot + n // 2, n)

    def project_q(slot, count):
        val = project(wqbuf[pl.ds(slot, count)].reshape(count * pair, ch))
        for n in range(count):
            keep(val, 2, slot + n, n)

    def remote(src, dst, sem_s, sem_r, rr, cc, core):
        return pltpu.make_async_remote_copy(
            src_ref=src, dst_ref=dst, send_sem=sem_s, recv_sem=sem_r,
            device_id=(z, rr, cc, core), device_id_type=MESH)

    def kv_send(i, g):
        rr, cc = chip_to(i)
        for b in range(2):
            for n, dst in ((0, k_all), (1, v_all)):
                remote(sbuf.at[n, i + 1, b], dst.at[i + 1, k], send_sem.at[0], kv_sem.at[g], rr, cc, b).start()

    def q_send(i):
        rr, cc = chip_to(i)
        for b in range(2):
            remote(sbuf.at[2, i + 1, b], q_all.at[i + 1, k], send_sem.at[0], q_sem.at[(i + 1) // 2], rr, cc, b).start()

    def kv_group(g, start, count):
        loaded(wbuf, 2 * (start + 1), 2 * count, w_sem.at[g])
        project_kv(start + 1, count)

    def kv_group_send(g, start, count):
        for n in range(count):
            kv_send(start + n, g)

    x_copy.wait()
    load_kv(2)
    kv_group(0, *groups[0])
    for g in range(3, n_group):
        load_kv(g)
    with jax.named_scope("barrier"):
        pl.semaphore_wait(barrier, 2 * n_step + 1)
    kv_group_send(0, *groups[0])
    kv_group(1, *groups[1])
    kv_group_send(1, *groups[1])

    def kv_loop(g, _):
        load_q(g - 2)
        start = (g - 2) * WIDE + groups[2][0]
        kv_group(g, start, WIDE)
        kv_group_send(g, start, WIDE)
        return 0

    with jax.named_scope("kv_loop"):
        lax.fori_loop(2, n_group, kv_loop, 0)

    for g in range(n_group - 2, n_q):
        load_q(g)
    kv_weights(own, my_chip, w_sem.at[n_group])
    q_weights(own, my_chip, w_sem.at[n_group])

    def q_loop(g, _):
        start = g * WIDE
        loaded(wqbuf, start + 1, WIDE, wq_sem.at[g])
        project_q(start + 1, WIDE)
        return 0

    with jax.named_scope("q_loop"):
        lax.fori_loop(0, n_q, q_loop, 0)

    def flip(slot):
        val = v_all[slot].reshape(2 * tok, pair)
        vt[:, slot * 2 * tok:(slot + 1) * 2 * tok] = val.T

    def kv_arrive(g):
        start, count = groups[g]
        part = sbuf.at[pl.ds(0, 2), pl.ds(start + 1, count)]
        pltpu.make_async_copy(part, part, kv_sem.at[g]).wait()
        for i in range(start, start + count):
            q_send(i)
        for i in range(start, start + count):
            flip(i + 1)

    kv_arrive(0)
    kv_arrive(1)

    with jax.named_scope("own"):
        pltpu.make_async_copy(wo_hbm.at[my_chip], wobuf.at[own], wo_sem).start()
        for i in range(n_step):
            pltpu.make_async_copy(wo_hbm.at[chip_id(i)], wobuf.at[i + 1], wo_sem).start()
        loaded(wbuf, 2 * own, 2, w_sem.at[n_group])
        loaded(wqbuf, own, 1, w_sem.at[n_group])
        project_kv(own, 1)
        project_q(own, 1)
        for n, dst in ((0, k_all), (1, v_all), (2, q_all)):
            dst[own, k] = sbuf[n, own, k]
            remote(sbuf.at[n, own, 1 - k], dst.at[own, k], send_sem.at[1], kv_sem.at[n_group], r, c, 1 - k).start()

    with jax.named_scope("kv_arrive"):
        for g in range(2, n_group):
            kv_arrive(g)
        part = sbuf.at[:, 0, 0]
        pltpu.make_async_copy(part, part, kv_sem.at[n_group]).wait()
        flip(own)

    def arrived(ref, slot, count, sem):
        part = ref.at[pl.ds(slot, count)]
        pltpu.make_async_copy(part, part, sem).wait()

    keys = chips * 2 * tok
    lanes = 4 * tok * UNIT
    n_unit = chips // UNIT

    def queries(unit):
        parts = []
        for u in range(UNIT):
            q = q_all[unit * UNIT + u].reshape(2 * tok, pair) * BF16(head**-0.5)
            first = lax.broadcasted_iota(jnp.int32, q.shape, 1) < head
            zero = jnp.zeros_like(q)
            parts += [jnp.where(first, q, zero), jnp.where(first, zero, q)]
        return jnp.concatenate(parts, axis=0)

    def scores(qq, scr, lo, n):
        keys_c = k_all[lo // (2 * tok):(lo + n) // (2 * tok)].reshape(n, pair)
        s = lax.dot_general(keys_c, qq, NT, preferred_element_type=F32)
        scr[lo:lo + n] = s
        return jnp.max(s.reshape(n // 8, 8, lanes), axis=0)

    def weigh(scr, top, lo, n):
        w = jnp.exp(scr[lo:lo + n] - top)
        part = jnp.sum(w.reshape(n // 8, 8, lanes), axis=0)
        return part, lax.dot_general(vt[:, lo:lo + n], w.astype(BF16), NN, preferred_element_type=F32)

    def both(scr, top, next_unit, next_scr):
        new_top = total = acc = None
        qq = None if next_unit is None else queries(next_unit)
        for at in range(0, keys, KEY_CHUNK):
            if qq is not None:
                high = scores(qq, next_scr, at, KEY_CHUNK)
                new_top = high if new_top is None else jnp.maximum(new_top, high)
            if scr is not None:
                part, piece = weigh(scr, top, at, KEY_CHUNK)
                total = part if total is None else total + part
                acc = piece if acc is None else acc + piece
        if qq is not None:
            new_top = jnp.max(new_top, axis=0, keepdims=True)
        outs = []
        if scr is not None:
            total = jnp.sum(total, axis=0, keepdims=True)
            wide = 2 * tok
            for u in range(UNIT):
                a, b, e = 2 * u * wide, (2 * u + 1) * wide, (2 * u + 2) * wide
                out = jnp.concatenate([acc[:head, a:b] / total[:, a:b], acc[head:, b:e] / total[:, b:e]], axis=0)
                outs.append(out.T.astype(BF16))
        return outs, new_top

    half_slots = chips // 2

    def put(slot, out):
        rr, cc = chip_from(slot - 1)
        for core in range(2):
            obuf[slot, core] = out[core * tok:(core + 1) * tok]
            remote(obuf.at[slot, core], ob.at[k, :, pl.ds(pl.multiple_of(slot * pair, pair), pair)],
                   send_sem.at[2], o_sem.at[slot // half_slots], rr, cc, core).start()

    def put_own(out):
        for core in range(2):
            obuf[own, core] = out[core * tok:(core + 1) * tok]
        at = pl.ds(own * pair, pair)
        ob[k, :, at] = obuf[own, k]
        remote(obuf.at[own, 1 - k], ob.at[k, :, at], send_sem.at[3], o_sem.at[2], r, c, 1 - k).start()

    def q_wait(unit):
        with jax.named_scope("q_wait"):
            arrived(q_all, 1, UNIT, q_sem.at[unit])

    def attend(j, top):
        unit = 2 * j + 1
        for scr, next_scr in ((s1, s0), (s0, s1)):
            q_wait(unit + 1)
            outs, top = both(scr, top, unit + 1, next_scr)
            for u in range(UNIT):
                put(unit * UNIT + u, outs[u])
            unit = unit + 1
        return top

    with jax.named_scope("q_first"):
        arrived(q_all, 1, 1, q_sem.at[0])
    _, top = both(None, None, 0, s0)
    q_wait(1)
    outs, top = both(s0, top, 1, s1)
    put_own(outs[0])
    put(1, outs[1])
    with jax.named_scope("attend"):
        top = lax.fori_loop(0, (n_unit - 2) // 2, attend, top)
    with jax.named_scope("last"):
        outs, _ = both(s1, top, None, None)
        for u in range(UNIT):
            put((n_unit - 1) * UNIT + u, outs[u])

    blk = 512

    def o_part(lo, hi, n):
        cs = pl.ds(pl.multiple_of(n * blk, blk), blk)
        lhs = ob[:, :, lo:hi].reshape(2 * tok, hi - lo)
        w = wobuf[lo // pair:hi // pair, :, cs].reshape(hi - lo, blk)
        return lax.dot_general(lhs, w, NN, preferred_element_type=F32), cs

    cut = half_slots * pair

    def o_first(n, _):
        y, cs = o_part(0, cut, n)
        s0[pl.ds(pl.multiple_of(n * 2 * tok, 2 * tok), 2 * tok), :] = y
        return 0

    def o_second(n, _):
        y, cs = o_part(cut, ch, n)
        at = pl.ds(pl.multiple_of(n * 2 * tok, 2 * tok), 2 * tok)
        y = y + s0[at, :]
        y_ref[:, cs] = y.astype(BF16)
        pltpu.make_async_copy(y_ref.at[:, cs], y_hbm.at[:, cs], y_sem).start()
        return 0

    with jax.named_scope("o_arrive1"):
        pltpu.make_async_copy(wo_hbm, wobuf, wo_sem).wait()
        pltpu.make_async_copy(obuf.at[0, 0], obuf.at[0, 0], o_sem.at[2]).wait()
        arrived(obuf, 1, half_slots - 1, o_sem.at[0])
    with jax.named_scope("o_first"):
        lax.fori_loop(0, ch // blk, o_first, 0)
    with jax.named_scope("o_arrive2"):
        arrived(obuf, half_slots, chips - half_slots, o_sem.at[1])
    with jax.named_scope("o_second"):
        lax.fori_loop(0, ch // blk, o_second, 0)

    with jax.named_scope("drain"):
        rest = sbuf.at[:, pl.ds(1, n_step)]
        pltpu.make_async_copy(rest, rest, send_sem.at[0]).wait()
        pltpu.make_async_copy(sbuf.at[:, 0, 0], sbuf.at[:, 0, 0], send_sem.at[1]).wait()
        arrived(obuf, 1, n_step, send_sem.at[2])
        pltpu.make_async_copy(obuf.at[0, 0], obuf.at[0, 0], send_sem.at[3]).wait()
        pltpu.make_async_copy(y_ref, y_hbm, y_sem).wait()


def solution(mesh):
    tok_spec = P("data", ("row", "col", "core"), None)
    rows, cols, cores = mesh.shape["row"], mesh.shape["col"], mesh.shape["core"]

    def per_device(tokens, w_qkv, w_out):
        batch, tok, ch = tokens.shape
        _, _, heads, head = w_qkv.shape
        chips = rows * cols
        pair = heads // chips * head
        dims = (rows, cols, tok, pair, head)
        keys = chips * cores * tok
        wt = jnp.transpose(w_qkv, (1, 2, 3, 0)).reshape(3 * chips, pair, ch)
        wo = w_out.reshape(chips, pair, ch)
        dma = pltpu.SemaphoreType.DMA
        n_group = len(groups_of(chips - 1))
        y = pl.pallas_call(
            functools.partial(kernel, dims),
            out_shape=jax.ShapeDtypeStruct((batch * tok, ch), BF16),
            in_specs=[pl.BlockSpec(memory_space=pl.ANY)] * 3,
            out_specs=pl.BlockSpec(memory_space=pl.ANY),
            scratch_shapes=[
                pltpu.VMEM((batch * tok, ch), BF16),
                pltpu.VMEM((2 * chips, pair, ch), BF16),
                pltpu.VMEM((chips, pair, ch), BF16),
                pltpu.VMEM((chips, pair, ch), BF16),
                pltpu.VMEM((3, chips, 2, tok, pair), BF16),
                pltpu.VMEM((chips, 2, tok, pair), BF16),
                pltpu.VMEM((chips, 2, tok, pair), BF16),
                pltpu.VMEM((chips, 2, tok, pair), BF16),
                pltpu.VMEM((pair, keys), BF16),
                pltpu.VMEM((keys, 4 * tok * UNIT), F32),
                pltpu.VMEM((keys, 4 * tok * UNIT), F32),
                pltpu.VMEM((chips, 2, tok, pair), BF16),
                pltpu.VMEM((2, tok, heads * head), BF16),
                pltpu.VMEM((batch * tok, ch), BF16),
                dma,
                dma((n_group + 1,)),
                dma(((chips - 1) // WIDE,)),
                dma,
                dma((4,)),
                dma((n_group + 1,)),
                dma((chips // 2,)),
                dma((3,)),
                dma,
            ],
            compiler_params=pltpu.CompilerParams(
                collective_id=0, has_side_effects=True, vmem_limit_bytes=60 * 1024 * 1024),
        )(tokens.reshape(batch * tok, ch), wt, wo)
        return y.reshape(batch, tok, ch)

    return jax.shard_map(per_device, mesh=mesh, in_specs=(tok_spec, P(), P()), out_specs=tok_spec, check_vma=False)
```

```python
import functools

import jax
import jax.numpy as jnp
from jax import lax
from jax.experimental import pallas as pl
from jax.experimental.pallas import tpu as pltpu
from jax.sharding import PartitionSpec as P

MESH = pl.DeviceIdType.MESH
F32 = jnp.float32
BF16 = jnp.bfloat16
NT = (((1,), (1,)), ((), ()))
NN = (((1,), (0,)), ((), ()))
KEY_CHUNK = 512
WIDE = 3
UNIT = 2
BLOCK = 512


def groups_of(n_step):
    sizes = [1, WIDE - 1] + [WIDE] * (n_step // WIDE - 1)
    starts = [sum(sizes[:g]) for g in range(len(sizes))]
    return list(zip(starts, sizes))


def hop_order(rows, cols):
    def hops(d, n):
        return min(d, n - d)

    offs = [(dy, dx) for dy in range(rows) for dx in range(cols)][1:]
    like = [[(2, 2)], [(1, 1), (3, 3)], [(2, 1), (2, 3), (0, 2)], [(1, 2), (3, 2), (2, 0)], [(1, 3), (3, 1), (0, 1)]]
    first = [o for group in like for o in group if o in offs]
    rest = [o for o in offs if o not in first]
    return first + sorted(rest, key=lambda o: -hops(o[0], rows) - hops(o[1], cols))


def pack_table(values, base):
    words = []
    for start in range(0, len(values), 8):
        words.append(sum(v * base**i for i, v in enumerate(values[start : start + 8])))
    return words


def kernel(dims, x_hbm, wt_hbm, wo_hbm, ob, wobuf, y_part, x_ref, wbuf, wqbuf, sbuf, k_all, v_all, q_all, vt, s0, s1, obuf,
           x_sem, w_sem, wq_sem, wo_sem, send_sem, kv_sem, q_sem, o_sem):
    rows, cols, tok, pair, head = dims
    chips = rows * cols
    ch = x_ref.shape[1]
    z = lax.axis_index("data")
    r = lax.axis_index("row")
    c = lax.axis_index("col")
    k = lax.axis_index("core")
    my_chip = r * cols + c
    order = hop_order(rows, cols)
    n_step = len(order)
    groups = groups_of(n_step)
    n_group = len(groups)
    own = 0
    dy_words = pack_table([o[0] for o in order], rows)
    dx_words = pack_table([o[1] for o in order], cols)

    def digit(words, base, i):
        val = words[0]
        for w, word in enumerate(words[1:]):
            val = val + (word - words[w]) * (jnp.minimum(i // (8 * (w + 1)), 1))
        shift = base.bit_length() - 1
        return lax.rem(lax.shift_right_logical(jnp.int32(0) + val, shift * lax.rem(i, 8)), base)

    def step_offset(i):
        if isinstance(i, int):
            return order[i]
        return digit(dy_words, rows, i), digit(dx_words, cols, i)

    def chip_to(i):
        dy, dx = step_offset(i)
        return lax.rem(r + dy, rows), lax.rem(c + dx, cols)

    def chip_from(i):
        dy, dx = step_offset(i)
        return lax.rem(r + rows - dy, rows), lax.rem(c + cols - dx, cols)

    x_copy = pltpu.make_async_copy(x_hbm, x_ref, x_sem)
    x_copy.start()

    def kv_weights(slot, chip, sem):
        for n in range(2):
            pltpu.make_async_copy(wt_hbm.at[(n + 1) * chips + chip], wbuf.at[2 * slot + n], sem).start()

    def q_weights(slot, chip, sem):
        pltpu.make_async_copy(wt_hbm.at[chip], wqbuf.at[slot], sem).start()

    def chip_id(i):
        rr, cc = chip_to(i)
        return rr * cols + cc

    n_q = n_step // WIDE

    def load_kv(g):
        start, count = groups[g]
        for i in range(start, start + count):
            kv_weights(i + 1, chip_id(i), w_sem.at[g])

    def load_q(g):
        for n in range(WIDE):
            i = g * WIDE + n
            q_weights(i + 1, chip_id(i), wq_sem.at[g])

    def loaded(ref, slot, count, sem):
        part = ref.at[pl.ds(slot, count)]
        pltpu.make_async_copy(part, part, sem).wait()

    load_kv(0)
    barrier = pltpu.get_barrier_semaphore()
    for i in range(n_step):
        rr, cc = chip_to(i)
        for core in range(2):
            pl.semaphore_signal(barrier, inc=1, device_id=(z, rr, cc, core), device_id_type=MESH)
    pl.semaphore_signal(barrier, inc=1, device_id=(z, r, c, 1 - k), device_id_type=MESH)

    load_kv(1)

    def project(w):
        return lax.dot_general(w, x_ref[...], NT, preferred_element_type=F32).astype(BF16).T

    def keep(val, piece, slot, n):
        for b in range(2):
            sbuf[piece, slot, b] = val[b * tok:(b + 1) * tok, n * pair:(n + 1) * pair]

    def project_kv(slot, count):
        val = project(wbuf[pl.ds(2 * slot, 2 * count)].reshape(2 * count * pair, ch))
        for n in range(2 * count):
            keep(val, n % 2, slot + n // 2, n)

    def project_q(slot, count):
        val = project(wqbuf[pl.ds(slot, count)].reshape(count * pair, ch))
        for n in range(count):
            keep(val, 2, slot + n, n)

    def remote(src, dst, sem_s, sem_r, rr, cc, core):
        return pltpu.make_async_remote_copy(
            src_ref=src, dst_ref=dst, send_sem=sem_s, recv_sem=sem_r,
            device_id=(z, rr, cc, core), device_id_type=MESH)

    def kv_send(i, g):
        rr, cc = chip_to(i)
        for b in range(2):
            for n, dst in ((0, k_all), (1, v_all)):
                remote(sbuf.at[n, i + 1, b], dst.at[i + 1, k], send_sem.at[0], kv_sem.at[g], rr, cc, b).start()

    def q_send(i):
        rr, cc = chip_to(i)
        for b in range(2):
            remote(sbuf.at[2, i + 1, b], q_all.at[i + 1, k], send_sem.at[0], q_sem.at[(i + 1) // 2], rr, cc, b).start()

    def kv_group(g, start, count):
        loaded(wbuf, 2 * (start + 1), 2 * count, w_sem.at[g])
        project_kv(start + 1, count)

    def kv_group_send(g, start, count):
        for n in range(count):
            kv_send(start + n, g)

    x_copy.wait()
    load_kv(2)
    kv_group(0, *groups[0])
    for g in range(3, n_group):
        load_kv(g)
    with jax.named_scope("barrier"):
        pl.semaphore_wait(barrier, 2 * n_step + 1)
    kv_group_send(0, *groups[0])
    kv_group(1, *groups[1])
    kv_group_send(1, *groups[1])

    def kv_loop(g, _):
        load_q(g - 2)
        start = (g - 2) * WIDE + groups[2][0]
        kv_group(g, start, WIDE)
        kv_group_send(g, start, WIDE)
        return 0

    with jax.named_scope("kv_loop"):
        lax.fori_loop(2, n_group, kv_loop, 0)

    for g in range(n_group - 2, n_q):
        load_q(g)
    kv_weights(own, my_chip, w_sem.at[n_group])
    q_weights(own, my_chip, w_sem.at[n_group])

    def q_loop(g, _):
        start = g * WIDE
        loaded(wqbuf, start + 1, WIDE, wq_sem.at[g])
        project_q(start + 1, WIDE)
        return 0

    with jax.named_scope("q_loop"):
        lax.fori_loop(0, n_q, q_loop, 0)

    def flip(slot):
        val = v_all[slot].reshape(2 * tok, pair)
        vt[:, slot * 2 * tok:(slot + 1) * 2 * tok] = val.T

    def kv_arrive(g):
        start, count = groups[g]
        part = sbuf.at[pl.ds(0, 2), pl.ds(start + 1, count)]
        pltpu.make_async_copy(part, part, kv_sem.at[g]).wait()
        for i in range(start, start + count):
            q_send(i)
        for i in range(start, start + count):
            flip(i + 1)

    kv_arrive(0)
    kv_arrive(1)

    with jax.named_scope("own"):
        pltpu.make_async_copy(wo_hbm.at[my_chip], wobuf.at[own], wo_sem).start()
        for i in range(n_step):
            pltpu.make_async_copy(wo_hbm.at[chip_id(i)], wobuf.at[i + 1], wo_sem).start()
        loaded(wbuf, 2 * own, 2, w_sem.at[n_group])
        loaded(wqbuf, own, 1, w_sem.at[n_group])
        project_kv(own, 1)
        project_q(own, 1)
        for n, dst in ((0, k_all), (1, v_all), (2, q_all)):
            dst[own, k] = sbuf[n, own, k]
            remote(sbuf.at[n, own, 1 - k], dst.at[own, k], send_sem.at[1], kv_sem.at[n_group], r, c, 1 - k).start()

    with jax.named_scope("kv_arrive"):
        for g in range(2, n_group):
            kv_arrive(g)
        part = sbuf.at[:, 0, 0]
        pltpu.make_async_copy(part, part, kv_sem.at[n_group]).wait()
        flip(own)

    def arrived(ref, slot, count, sem):
        part = ref.at[pl.ds(slot, count)]
        pltpu.make_async_copy(part, part, sem).wait()

    keys = chips * 2 * tok
    lanes = 4 * tok * UNIT
    n_unit = chips // UNIT

    def queries(unit):
        parts = []
        for u in range(UNIT):
            q = q_all[unit * UNIT + u].reshape(2 * tok, pair) * BF16(head**-0.5)
            first = lax.broadcasted_iota(jnp.int32, q.shape, 1) < head
            zero = jnp.zeros_like(q)
            parts += [jnp.where(first, q, zero), jnp.where(first, zero, q)]
        return jnp.concatenate(parts, axis=0)

    def scores(qq, scr, lo, n):
        keys_c = k_all[lo // (2 * tok):(lo + n) // (2 * tok)].reshape(n, pair)
        s = lax.dot_general(keys_c, qq, NT, preferred_element_type=F32)
        scr[lo:lo + n] = s
        return jnp.max(s.reshape(n // 8, 8, lanes), axis=0)

    def weigh(scr, top, lo, n):
        w = jnp.exp(scr[lo:lo + n] - top)
        part = jnp.sum(w.reshape(n // 8, 8, lanes), axis=0)
        return part, lax.dot_general(vt[:, lo:lo + n], w.astype(BF16), NN, preferred_element_type=F32)

    def both(scr, top, next_unit, next_scr):
        new_top = total = acc = None
        qq = None if next_unit is None else queries(next_unit)
        for at in range(0, keys, KEY_CHUNK):
            if qq is not None:
                high = scores(qq, next_scr, at, KEY_CHUNK)
                new_top = high if new_top is None else jnp.maximum(new_top, high)
            if scr is not None:
                part, piece = weigh(scr, top, at, KEY_CHUNK)
                total = part if total is None else total + part
                acc = piece if acc is None else acc + piece
        if qq is not None:
            new_top = jnp.max(new_top, axis=0, keepdims=True)
        outs = []
        if scr is not None:
            total = jnp.sum(total, axis=0, keepdims=True)
            wide = 2 * tok
            for u in range(UNIT):
                a, b, e = 2 * u * wide, (2 * u + 1) * wide, (2 * u + 2) * wide
                out = jnp.concatenate([acc[:head, a:b] / total[:, a:b], acc[head:, b:e] / total[:, b:e]], axis=0)
                outs.append(out.T.astype(BF16))
        return outs, new_top

    half_slots = chips // 2

    def put(slot, out):
        rr, cc = chip_from(slot - 1)
        for core in range(2):
            obuf[slot, core] = out[core * tok:(core + 1) * tok]
            remote(obuf.at[slot, core], ob.at[k, :, pl.ds(pl.multiple_of(slot * pair, pair), pair)],
                   send_sem.at[2], o_sem.at[slot // half_slots], rr, cc, core).start()

    def put_own(out):
        for core in range(2):
            obuf[own, core] = out[core * tok:(core + 1) * tok]
        at = pl.ds(own * pair, pair)
        ob[k, :, at] = obuf[own, k]
        remote(obuf.at[own, 1 - k], ob.at[k, :, at], send_sem.at[3], o_sem.at[2], r, c, 1 - k).start()

    def q_wait(unit):
        with jax.named_scope("q_wait"):
            arrived(q_all, 1, UNIT, q_sem.at[unit])

    def attend(j, top):
        unit = 2 * j + 1
        for scr, next_scr in ((s1, s0), (s0, s1)):
            q_wait(unit + 1)
            outs, top = both(scr, top, unit + 1, next_scr)
            for u in range(UNIT):
                put(unit * UNIT + u, outs[u])
            unit = unit + 1
        return top

    with jax.named_scope("q_first"):
        arrived(q_all, 1, 1, q_sem.at[0])
    _, top = both(None, None, 0, s0)
    q_wait(1)
    outs, top = both(s0, top, 1, s1)
    put_own(outs[0])
    put(1, outs[1])
    with jax.named_scope("attend"):
        top = lax.fori_loop(0, (n_unit - 2) // 2, attend, top)
    with jax.named_scope("last"):
        outs, _ = both(s1, top, None, None)
        for u in range(UNIT):
            put((n_unit - 1) * UNIT + u, outs[u])

    blk = BLOCK
    cut = half_slots * pair

    def o_first(n, _):
        cs = pl.ds(pl.multiple_of(n * blk, blk), blk)
        lhs = ob[:, :, :cut].reshape(2 * tok, cut)
        w = wobuf[:half_slots, :, cs].reshape(cut, blk)
        y_part[:, cs] = lax.dot_general(lhs, w, NN, preferred_element_type=F32)
        return 0

    with jax.named_scope("o_arrive1"):
        pltpu.make_async_copy(wo_hbm, wobuf, wo_sem).wait()
        pltpu.make_async_copy(obuf.at[0, 0], obuf.at[0, 0], o_sem.at[2]).wait()
        arrived(obuf, 1, half_slots - 1, o_sem.at[0])
    with jax.named_scope("o_first"):
        lax.fori_loop(0, ch // blk, o_first, 0)
    with jax.named_scope("drain"):
        rest = sbuf.at[:, pl.ds(1, n_step)]
        pltpu.make_async_copy(rest, rest, send_sem.at[0]).wait()
        pltpu.make_async_copy(sbuf.at[:, 0, 0], sbuf.at[:, 0, 0], send_sem.at[1]).wait()
        pltpu.make_async_copy(obuf.at[0, 0], obuf.at[0, 0], send_sem.at[3]).wait()
        arrived(obuf, 1, n_step, send_sem.at[2])
    with jax.named_scope("o_arrive2"):
        arrived(obuf, half_slots, chips - half_slots, o_sem.at[1])


def finish_kernel(ob, wobuf, y_part, y_hbm, y_ref, y_sem):
    _, tok, width = ob.shape
    chips, pair, ch = wobuf.shape
    half, cut = chips // 2, width // 2

    def second(n, _):
        cs = pl.ds(pl.multiple_of(n * BLOCK, BLOCK), BLOCK)
        lhs = ob[:, :, cut:].reshape(2 * tok, width - cut)
        w = wobuf[half:, :, cs].reshape(width - cut, BLOCK)
        y = y_part[:, cs] + lax.dot_general(lhs, w, NN, preferred_element_type=F32)
        y_ref[:, cs] = y.astype(BF16)
        pltpu.make_async_copy(y_ref.at[:, cs], y_hbm.at[:, cs], y_sem).start()
        return 0

    lax.fori_loop(0, ch // BLOCK, second, 0)
    pltpu.make_async_copy(y_ref, y_hbm, y_sem).wait()


def solution(mesh):
    tok_spec = P("data", ("row", "col", "core"), None)
    rows, cols, cores = mesh.shape["row"], mesh.shape["col"], mesh.shape["core"]

    def per_device(tokens, w_qkv, w_out):
        batch, tok, ch = tokens.shape
        _, _, heads, head = w_qkv.shape
        chips = rows * cols
        pair = heads // chips * head
        dims = (rows, cols, tok, pair, head)
        keys = chips * cores * tok
        wt = jnp.transpose(w_qkv, (1, 2, 3, 0)).reshape(3 * chips, pair, ch)
        wo = w_out.reshape(chips, pair, ch)
        dma = pltpu.SemaphoreType.DMA
        n_group = len(groups_of(chips - 1))
        vmem = pl.BlockSpec(memory_space=pltpu.VMEM)
        ob, wobuf, y_part = pl.pallas_call(
            functools.partial(kernel, dims),
            out_shape=(
                pltpu.VMEM((2, tok, heads * head), BF16),
                pltpu.VMEM((chips, pair, ch), BF16),
                pltpu.VMEM((batch * tok, ch), F32),
            ),
            in_specs=[pl.BlockSpec(memory_space=pl.ANY)] * 3,
            out_specs=(vmem, vmem, vmem),
            scratch_shapes=[
                pltpu.VMEM((batch * tok, ch), BF16),
                pltpu.VMEM((2 * chips, pair, ch), BF16),
                pltpu.VMEM((chips, pair, ch), BF16),
                pltpu.VMEM((3, chips, 2, tok, pair), BF16),
                pltpu.VMEM((chips, 2, tok, pair), BF16),
                pltpu.VMEM((chips, 2, tok, pair), BF16),
                pltpu.VMEM((chips, 2, tok, pair), BF16),
                pltpu.VMEM((pair, keys), BF16),
                pltpu.VMEM((keys, 4 * tok * UNIT), F32),
                pltpu.VMEM((keys, 4 * tok * UNIT), F32),
                pltpu.VMEM((chips, 2, tok, pair), BF16),
                dma,
                dma((n_group + 1,)),
                dma(((chips - 1) // WIDE,)),
                dma,
                dma((4,)),
                dma((n_group + 1,)),
                dma((chips // 2,)),
                dma((3,)),
            ],
            compiler_params=pltpu.CompilerParams(
                collective_id=0, has_side_effects=True, vmem_limit_bytes=44 * 1024 * 1024),
        )(tokens.reshape(batch * tok, ch), wt, wo)
        y = pl.pallas_call(
            finish_kernel,
            out_shape=jax.ShapeDtypeStruct((batch * tok, ch), BF16),
            in_specs=[vmem] * 3,
            out_specs=pl.BlockSpec(memory_space=pl.ANY),
            scratch_shapes=[pltpu.VMEM((batch * tok, ch), BF16), dma],
            compiler_params=pltpu.CompilerParams(vmem_limit_bytes=8 * 1024 * 1024),
        )(ob, wobuf, y_part)
        return y.reshape(batch, tok, ch)

    return jax.shard_map(per_device, mesh=mesh, in_specs=(tok_spec, P(), P()), out_specs=tok_spec, check_vma=False)
```

```python
import functools

import jax
import jax.numpy as jnp
from jax import lax
from jax.experimental import pallas as pl
from jax.experimental.pallas import tpu as pltpu
from jax.sharding import PartitionSpec as P

MESH = pl.DeviceIdType.MESH
F32 = jnp.float32
BF16 = jnp.bfloat16
NT = (((1,), (1,)), ((), ()))
NN = (((1,), (0,)), ((), ()))
KEY_CHUNK = 512
WIDE = 3
UNIT = 2
BLOCK = 2048


def groups_of(n_step):
    sizes = [1, WIDE - 1] + [WIDE] * (n_step // WIDE - 1)
    starts = [sum(sizes[:g]) for g in range(len(sizes))]
    return list(zip(starts, sizes))


def hop_order(rows, cols):
    def hops(d, n):
        return min(d, n - d)

    offs = [(dy, dx) for dy in range(rows) for dx in range(cols)][1:]
    like = [[(2, 2)], [(1, 1), (3, 3)], [(2, 1), (2, 3), (0, 2)], [(1, 2), (3, 2), (2, 0)], [(1, 3), (3, 1), (0, 1)]]
    first = [o for group in like for o in group if o in offs]
    rest = [o for o in offs if o not in first]
    return first + sorted(rest, key=lambda o: -hops(o[0], rows) - hops(o[1], cols))


def query_order(rows, cols):
    def hops(d, n):
        return min(d, n - d)

    offs = [(dy, dx) for dy in range(rows) for dx in range(cols)][1:]
    near, mid, far = ([o for o in offs if lo <= hops(o[0], rows) + hops(o[1], cols) <= hi] for lo, hi in ((1, 1), (2, 2), (3, 4)))
    return near[:3] + mid[:2] + far + mid[2:] + near[3:]


def pack_table(values, base):
    words = []
    for start in range(0, len(values), 8):
        words.append(sum(v * base**i for i, v in enumerate(values[start : start + 8])))
    return words


def kernel(dims, x_hbm, wt_hbm, wo_hbm, ob, wobuf, y_part, x_ref, wbuf, wqbuf, sbuf, k_all, v_all, q_all, vt, s0, s1, obuf,
           x_sem, w_sem, wq_sem, wo_sem, send_sem, kv_sem, q_sem, o_sem):
    rows, cols, tok, pair, head = dims
    chips = rows * cols
    ch = x_ref.shape[1]
    z = lax.axis_index("data")
    r = lax.axis_index("row")
    c = lax.axis_index("col")
    k = lax.axis_index("core")
    my_chip = r * cols + c
    order = hop_order(rows, cols)
    q_order = query_order(rows, cols)
    n_step = len(order)
    groups = groups_of(n_step)
    n_group = len(groups)
    own = 0
    q_own = n_step
    words = {id(o): (pack_table([d[0] for d in o], rows), pack_table([d[1] for d in o], cols)) for o in (order, q_order)}

    def digit(table, base, i):
        val = table[0]
        for w, word in enumerate(table[1:]):
            val = val + (word - table[w]) * (jnp.minimum(i // (8 * (w + 1)), 1))
        shift = base.bit_length() - 1
        return lax.rem(lax.shift_right_logical(jnp.int32(0) + val, shift * lax.rem(i, 8)), base)

    def offset(i, table):
        if isinstance(i, int):
            return table[i]
        dy_words, dx_words = words[id(table)]
        return digit(dy_words, rows, i), digit(dx_words, cols, i)

    def chip_to(i, table=order):
        dy, dx = offset(i, table)
        return lax.rem(r + dy, rows), lax.rem(c + dx, cols)

    def chip_from(i, table=order):
        dy, dx = offset(i, table)
        return lax.rem(r + rows - dy, rows), lax.rem(c + cols - dx, cols)

    x_copy = pltpu.make_async_copy(x_hbm, x_ref, x_sem)
    x_copy.start()

    def kv_weights(slot, chip, sem):
        for n in range(2):
            pltpu.make_async_copy(wt_hbm.at[(n + 1) * chips + chip], wbuf.at[2 * slot + n], sem).start()

    def q_weights(slot, chip, sem):
        pltpu.make_async_copy(wt_hbm.at[chip], wqbuf.at[slot], sem).start()

    def chip_id(i, table=order):
        rr, cc = chip_to(i, table)
        return rr * cols + cc

    n_q = n_step // WIDE

    def load_kv(g):
        start, count = groups[g]
        for i in range(start, start + count):
            kv_weights(i + 1, chip_id(i), w_sem.at[g])

    def load_q(g):
        for n in range(WIDE):
            i = g * WIDE + n
            q_weights(i, chip_id(i, q_order), wq_sem.at[g])

    def loaded(ref, slot, count, sem):
        part = ref.at[pl.ds(slot, count)]
        pltpu.make_async_copy(part, part, sem).wait()

    load_kv(0)
    barrier = pltpu.get_barrier_semaphore()
    for i in range(n_step):
        rr, cc = chip_to(i)
        for core in range(2):
            pl.semaphore_signal(barrier, inc=1, device_id=(z, rr, cc, core), device_id_type=MESH)
    pl.semaphore_signal(barrier, inc=1, device_id=(z, r, c, 1 - k), device_id_type=MESH)

    load_kv(1)

    def project(w):
        return lax.dot_general(w, x_ref[...], NT, preferred_element_type=F32).astype(BF16).T

    def keep(val, piece, slot, n):
        for b in range(2):
            sbuf[piece, slot, b] = val[b * tok:(b + 1) * tok, n * pair:(n + 1) * pair]

    def project_kv(slot, count):
        val = project(wbuf[pl.ds(2 * slot, 2 * count)].reshape(2 * count * pair, ch))
        for n in range(2 * count):
            keep(val, n % 2, slot + n // 2, n)

    def project_q(slot, count):
        val = project(wqbuf[pl.ds(slot, count)].reshape(count * pair, ch))
        for n in range(count):
            keep(val, 2, slot + n, n)

    def remote(src, dst, sem_s, sem_r, rr, cc, core):
        return pltpu.make_async_remote_copy(
            src_ref=src, dst_ref=dst, send_sem=sem_s, recv_sem=sem_r,
            device_id=(z, rr, cc, core), device_id_type=MESH)

    def kv_send(i, g):
        rr, cc = chip_to(i)
        for b in range(2):
            for n, dst in ((0, k_all), (1, v_all)):
                remote(sbuf.at[n, i + 1, b], dst.at[i + 1, k], send_sem.at[0], kv_sem.at[g], rr, cc, b).start()

    def q_send(i):
        rr, cc = chip_to(i, q_order)
        for b in range(2):
            remote(sbuf.at[2, i, b], q_all.at[i, k], send_sem.at[0], q_sem.at[i // UNIT], rr, cc, b).start()

    def kv_group(g, start, count):
        loaded(wbuf, 2 * (start + 1), 2 * count, w_sem.at[g])
        project_kv(start + 1, count)

    def kv_group_send(g, start, count):
        for n in range(count):
            kv_send(start + n, g)

    x_copy.wait()
    load_kv(2)
    kv_group(0, *groups[0])
    for g in range(3, n_group):
        load_kv(g)
    with jax.named_scope("barrier"):
        pl.semaphore_wait(barrier, 2 * n_step + 1)
    kv_group_send(0, *groups[0])
    kv_group(1, *groups[1])
    kv_group_send(1, *groups[1])

    def kv_loop(g, _):
        load_q(g - 2)
        start = (g - 2) * WIDE + groups[2][0]
        kv_group(g, start, WIDE)
        kv_group_send(g, start, WIDE)
        return 0

    with jax.named_scope("kv_loop"):
        lax.fori_loop(2, n_group, kv_loop, 0)

    for g in range(n_group - 2, n_q):
        load_q(g)
    kv_weights(own, my_chip, w_sem.at[n_group])
    q_weights(q_own, my_chip, w_sem.at[n_group])

    def q_loop(g, _):
        start = g * WIDE
        loaded(wqbuf, start, WIDE, wq_sem.at[g])
        project_q(start, WIDE)
        return 0

    with jax.named_scope("q_loop"):
        lax.fori_loop(0, n_q, q_loop, 0)

    def flip(slot):
        val = v_all[slot].reshape(2 * tok, pair)
        vt[:, slot * 2 * tok:(slot + 1) * 2 * tok] = val.T

    def kv_arrive(g):
        start, count = groups[g]
        part = sbuf.at[pl.ds(0, 2), pl.ds(start + 1, count)]
        pltpu.make_async_copy(part, part, kv_sem.at[g]).wait()
        for i in range(start, start + count):
            q_send(i)
        for i in range(start, start + count):
            flip(i + 1)

    kv_arrive(0)
    kv_arrive(1)

    with jax.named_scope("own"):
        for i in range(n_step):
            pltpu.make_async_copy(wo_hbm.at[chip_id(i, q_order)], wobuf.at[i], wo_sem).start()
        pltpu.make_async_copy(wo_hbm.at[my_chip], wobuf.at[q_own], wo_sem).start()
        loaded(wbuf, 2 * own, 2, w_sem.at[n_group])
        loaded(wqbuf, q_own, 1, w_sem.at[n_group])
        project_kv(own, 1)
        project_q(q_own, 1)
        for n, dst, at in ((0, k_all, own), (1, v_all, own), (2, q_all, q_own)):
            dst[at, k] = sbuf[n, at, k]
            remote(sbuf.at[n, at, 1 - k], dst.at[at, k], send_sem.at[1], kv_sem.at[n_group], r, c, 1 - k).start()

    with jax.named_scope("kv_arrive"):
        for g in range(2, n_group):
            kv_arrive(g)
        part = sbuf.at[:, 0, 0]
        pltpu.make_async_copy(part, part, kv_sem.at[n_group]).wait()
        flip(own)

    def arrived(ref, slot, count, sem):
        part = ref.at[pl.ds(slot, count)]
        pltpu.make_async_copy(part, part, sem).wait()

    keys = chips * 2 * tok
    lanes = 4 * tok * UNIT
    n_unit = chips // UNIT

    def queries(unit):
        parts = []
        for u in range(UNIT):
            q = q_all[unit * UNIT + u].reshape(2 * tok, pair) * BF16(head**-0.5)
            first = lax.broadcasted_iota(jnp.int32, q.shape, 1) < head
            zero = jnp.zeros_like(q)
            parts += [jnp.where(first, q, zero), jnp.where(first, zero, q)]
        return jnp.concatenate(parts, axis=0)

    def scores(qq, scr, lo, n):
        keys_c = k_all[lo // (2 * tok):(lo + n) // (2 * tok)].reshape(n, pair)
        s = lax.dot_general(keys_c, qq, NT, preferred_element_type=F32)
        scr[lo:lo + n] = s
        return jnp.max(s.reshape(n // 8, 8, lanes), axis=0)

    def weigh(scr, top, lo, n):
        w = jnp.exp(scr[lo:lo + n] - top)
        part = jnp.sum(w.reshape(n // 8, 8, lanes), axis=0)
        return part, lax.dot_general(vt[:, lo:lo + n], w.astype(BF16), NN, preferred_element_type=F32)

    def both(scr, top, next_unit, next_scr):
        new_top = total = acc = None
        qq = None if next_unit is None else queries(next_unit)
        for at in range(0, keys, KEY_CHUNK):
            if qq is not None:
                high = scores(qq, next_scr, at, KEY_CHUNK)
                new_top = high if new_top is None else jnp.maximum(new_top, high)
            if scr is not None:
                part, piece = weigh(scr, top, at, KEY_CHUNK)
                total = part if total is None else total + part
                acc = piece if acc is None else acc + piece
        if qq is not None:
            new_top = jnp.max(new_top, axis=0, keepdims=True)
        outs = []
        if scr is not None:
            total = jnp.sum(total, axis=0, keepdims=True)
            wide = 2 * tok
            for u in range(UNIT):
                a, b, e = 2 * u * wide, (2 * u + 1) * wide, (2 * u + 2) * wide
                out = jnp.concatenate([acc[:head, a:b] / total[:, a:b], acc[head:, b:e] / total[:, b:e]], axis=0)
                outs.append(out.T.astype(BF16))
        return outs, new_top

    half_slots = chips // 2

    def put(slot, out):
        rr, cc = chip_from(slot, q_order)
        for core in range(2):
            obuf[slot, core] = out[core * tok:(core + 1) * tok]
            remote(obuf.at[slot, core], ob.at[k, :, pl.ds(pl.multiple_of(slot * pair, pair), pair)],
                   send_sem.at[2], o_sem.at[slot // half_slots], rr, cc, core).start()

    def put_own(out):
        for core in range(2):
            obuf[q_own, core] = out[core * tok:(core + 1) * tok]
        at = pl.ds(q_own * pair, pair)
        ob[k, :, at] = obuf[q_own, k]
        remote(obuf.at[q_own, 1 - k], ob.at[k, :, at], send_sem.at[3], o_sem.at[2], r, c, 1 - k).start()

    def q_wait(unit, count=UNIT):
        with jax.named_scope("q_wait"):
            arrived(q_all, 0, count, q_sem.at[unit])

    def attend(j, top):
        unit = 2 * j
        for scr, next_scr in ((s0, s1), (s1, s0)):
            q_wait(unit + 1)
            outs, top = both(scr, top, unit + 1, next_scr)
            for u in range(UNIT):
                put(unit * UNIT + u, outs[u])
            unit = unit + 1
        return top

    q_wait(0)
    _, top = both(None, None, 0, s0)
    with jax.named_scope("attend"):
        top = lax.fori_loop(0, (n_unit - 2) // 2, attend, top)
    with jax.named_scope("last"):
        q_wait(n_unit - 1, UNIT - 1)
        outs, top = both(s0, top, n_unit - 1, s1)
        for u in range(UNIT):
            put((n_unit - 2) * UNIT + u, outs[u])
        outs, _ = both(s1, top, None, None)
        put(q_own - 1, outs[0])
        put_own(outs[1])

    blk = BLOCK
    cut = half_slots * pair

    def o_first(n, _):
        cs = pl.ds(pl.multiple_of(n * blk, blk), blk)
        lhs = ob[:, :, :cut].reshape(2 * tok, cut)
        w = wobuf[:half_slots, :, cs].reshape(cut, blk)
        y_part[:, cs] = lax.dot_general(lhs, w, NN, preferred_element_type=F32)
        return 0

    with jax.named_scope("o_arrive1"):
        pltpu.make_async_copy(wo_hbm, wobuf, wo_sem).wait()
        arrived(obuf, 0, half_slots, o_sem.at[0])
    with jax.named_scope("o_first"):
        lax.fori_loop(0, ch // blk, o_first, 0)
    with jax.named_scope("drain"):
        rest = sbuf.at[:, pl.ds(1, n_step)]
        pltpu.make_async_copy(rest, rest, send_sem.at[0]).wait()
        pltpu.make_async_copy(sbuf.at[:, 0, 0], sbuf.at[:, 0, 0], send_sem.at[1]).wait()
        pltpu.make_async_copy(obuf.at[0, 0], obuf.at[0, 0], send_sem.at[3]).wait()
        arrived(obuf, 0, n_step, send_sem.at[2])
    with jax.named_scope("o_arrive2"):
        arrived(obuf, half_slots, n_step - half_slots, o_sem.at[1])
        pltpu.make_async_copy(obuf.at[0, 0], obuf.at[0, 0], o_sem.at[2]).wait()


def finish_kernel(ob, wobuf, y_part, y_hbm, y_ref, y_sem):
    _, tok, width = ob.shape
    chips, pair, ch = wobuf.shape
    half, cut = chips // 2, width // 2

    def second(n, _):
        cs = pl.ds(pl.multiple_of(n * BLOCK, BLOCK), BLOCK)
        lhs = ob[:, :, cut:].reshape(2 * tok, width - cut)
        w = wobuf[half:, :, cs].reshape(width - cut, BLOCK)
        y = y_part[:, cs] + lax.dot_general(lhs, w, NN, preferred_element_type=F32)
        y_ref[:, cs] = y.astype(BF16)
        pltpu.make_async_copy(y_ref.at[:, cs], y_hbm.at[:, cs], y_sem).start()
        return 0

    lax.fori_loop(0, ch // BLOCK, second, 0)
    pltpu.make_async_copy(y_ref, y_hbm, y_sem).wait()


def solution(mesh):
    tok_spec = P("data", ("row", "col", "core"), None)
    rows, cols, cores = mesh.shape["row"], mesh.shape["col"], mesh.shape["core"]

    def per_device(tokens, w_qkv, w_out):
        batch, tok, ch = tokens.shape
        _, _, heads, head = w_qkv.shape
        chips = rows * cols
        pair = heads // chips * head
        dims = (rows, cols, tok, pair, head)
        keys = chips * cores * tok
        wt = jnp.transpose(w_qkv, (1, 2, 3, 0)).reshape(3 * chips, pair, ch)
        wo = w_out.reshape(chips, pair, ch)
        dma = pltpu.SemaphoreType.DMA
        n_group = len(groups_of(chips - 1))
        vmem = pl.BlockSpec(memory_space=pltpu.VMEM)
        ob, wobuf, y_part = pl.pallas_call(
            functools.partial(kernel, dims),
            out_shape=(
                pltpu.VMEM((2, tok, heads * head), BF16),
                pltpu.VMEM((chips, pair, ch), BF16),
                pltpu.VMEM((batch * tok, ch), F32),
            ),
            in_specs=[pl.BlockSpec(memory_space=pl.ANY)] * 3,
            out_specs=(vmem, vmem, vmem),
            scratch_shapes=[
                pltpu.VMEM((batch * tok, ch), BF16),
                pltpu.VMEM((2 * chips, pair, ch), BF16),
                pltpu.VMEM((chips, pair, ch), BF16),
                pltpu.VMEM((3, chips, 2, tok, pair), BF16),
                pltpu.VMEM((chips, 2, tok, pair), BF16),
                pltpu.VMEM((chips, 2, tok, pair), BF16),
                pltpu.VMEM((chips, 2, tok, pair), BF16),
                pltpu.VMEM((pair, keys), BF16),
                pltpu.VMEM((keys, 4 * tok * UNIT), F32),
                pltpu.VMEM((keys, 4 * tok * UNIT), F32),
                pltpu.VMEM((chips, 2, tok, pair), BF16),
                dma,
                dma((n_group + 1,)),
                dma(((chips - 1) // WIDE,)),
                dma,
                dma((4,)),
                dma((n_group + 1,)),
                dma((chips // 2,)),
                dma((3,)),
            ],
            compiler_params=pltpu.CompilerParams(
                collective_id=0, has_side_effects=True, vmem_limit_bytes=44 * 1024 * 1024),
        )(tokens.reshape(batch * tok, ch), wt, wo)
        y = pl.pallas_call(
            finish_kernel,
            out_shape=jax.ShapeDtypeStruct((batch * tok, ch), BF16),
            in_specs=[vmem] * 3,
            out_specs=pl.BlockSpec(memory_space=pl.ANY),
            scratch_shapes=[pltpu.VMEM((batch * tok, ch), BF16), dma],
            compiler_params=pltpu.CompilerParams(vmem_limit_bytes=8 * 1024 * 1024),
        )(ob, wobuf, y_part)
        return y.reshape(batch, tok, ch)

    return jax.shard_map(per_device, mesh=mesh, in_specs=(tok_spec, P(), P()), out_specs=tok_spec, check_vma=False)
```

```python
import functools

import jax
import jax.numpy as jnp
from jax import lax
from jax.experimental import pallas as pl
from jax.experimental.pallas import tpu as pltpu
from jax.sharding import PartitionSpec as P

MESH = pl.DeviceIdType.MESH
F32 = jnp.float32
BF16 = jnp.bfloat16
NT = (((1,), (1,)), ((), ()))
NN = (((1,), (0,)), ((), ()))
KEY_CHUNK = 512
WIDE = 3
UNIT = 2
BLOCK = 2048


def groups_of(n_step):
    sizes = [1, WIDE - 1] + [WIDE] * (n_step // WIDE - 1)
    starts = [sum(sizes[:g]) for g in range(len(sizes))]
    return list(zip(starts, sizes))


def hop_order(rows, cols):
    def hops(d, n):
        return min(d, n - d)

    offs = [(dy, dx) for dy in range(rows) for dx in range(cols)][1:]
    like = [[(2, 2)], [(1, 1), (3, 3)], [(2, 1), (2, 3), (0, 2)], [(1, 2), (3, 2), (2, 0)], [(1, 3), (3, 1), (0, 1)]]
    first = [o for group in like for o in group if o in offs]
    rest = [o for o in offs if o not in first]
    return first + sorted(rest, key=lambda o: -hops(o[0], rows) - hops(o[1], cols))


def query_order(rows, cols):
    def hops(d, n):
        return min(d, n - d)

    offs = [(dy, dx) for dy in range(rows) for dx in range(cols)][1:]
    near, mid, far = ([o for o in offs if lo <= hops(o[0], rows) + hops(o[1], cols) <= hi] for lo, hi in ((1, 1), (2, 2), (3, 4)))
    return near[:3] + mid + far + near[3:]


def pack_table(values, base):
    words = []
    for start in range(0, len(values), 8):
        words.append(sum(v * base**i for i, v in enumerate(values[start : start + 8])))
    return words


def kernel(dims, x_hbm, wt_hbm, wo_hbm, ob, wobuf, y_part, x_ref, wbuf, wqbuf, sbuf, k_all, v_all, q_all, vt, s0, s1, obuf,
           x_sem, w_sem, wq_sem, wo_sem, send_sem, kv_sem, q_sem, o_sem):
    rows, cols, tok, pair, head = dims
    chips = rows * cols
    ch = x_ref.shape[1]
    z = lax.axis_index("data")
    r = lax.axis_index("row")
    c = lax.axis_index("col")
    k = lax.axis_index("core")
    my_chip = r * cols + c
    order = hop_order(rows, cols)
    q_order = query_order(rows, cols)
    n_step = len(order)
    groups = groups_of(n_step)
    n_group = len(groups)
    own = 0
    q_own = n_step
    words = {id(o): (pack_table([d[0] for d in o], rows), pack_table([d[1] for d in o], cols)) for o in (order, q_order)}

    def digit(table, base, i):
        val = table[0]
        for w, word in enumerate(table[1:]):
            val = val + (word - table[w]) * (jnp.minimum(i // (8 * (w + 1)), 1))
        shift = base.bit_length() - 1
        return lax.rem(lax.shift_right_logical(jnp.int32(0) + val, shift * lax.rem(i, 8)), base)

    def offset(i, table):
        if isinstance(i, int):
            return table[i]
        dy_words, dx_words = words[id(table)]
        return digit(dy_words, rows, i), digit(dx_words, cols, i)

    def chip_to(i, table=order):
        dy, dx = offset(i, table)
        return lax.rem(r + dy, rows), lax.rem(c + dx, cols)

    def chip_from(i, table=order):
        dy, dx = offset(i, table)
        return lax.rem(r + rows - dy, rows), lax.rem(c + cols - dx, cols)

    x_copy = pltpu.make_async_copy(x_hbm, x_ref, x_sem)
    x_copy.start()

    def kv_weights(slot, chip, sem):
        for n in range(2):
            pltpu.make_async_copy(wt_hbm.at[(n + 1) * chips + chip], wbuf.at[2 * slot + n], sem).start()

    def q_weights(slot, chip, sem):
        pltpu.make_async_copy(wt_hbm.at[chip], wqbuf.at[slot], sem).start()

    def chip_id(i, table=order):
        rr, cc = chip_to(i, table)
        return rr * cols + cc

    n_q = n_step // WIDE

    def load_kv(g):
        start, count = groups[g]
        for i in range(start, start + count):
            kv_weights(i + 1, chip_id(i), w_sem.at[g])

    def load_q(g):
        for n in range(WIDE):
            i = g * WIDE + n
            q_weights(i, chip_id(i, q_order), wq_sem.at[g])

    def loaded(ref, slot, count, sem):
        part = ref.at[pl.ds(slot, count)]
        pltpu.make_async_copy(part, part, sem).wait()

    load_kv(0)
    barrier = pltpu.get_barrier_semaphore()
    for i in range(n_step):
        rr, cc = chip_to(i)
        for core in range(2):
            pl.semaphore_signal(barrier, inc=1, device_id=(z, rr, cc, core), device_id_type=MESH)
    pl.semaphore_signal(barrier, inc=1, device_id=(z, r, c, 1 - k), device_id_type=MESH)

    load_kv(1)

    def project(w):
        return lax.dot_general(w, x_ref[...], NT, preferred_element_type=F32).astype(BF16).T

    def keep(val, piece, slot, n):
        for b in range(2):
            sbuf[piece, slot, b] = val[b * tok:(b + 1) * tok, n * pair:(n + 1) * pair]

    def project_kv(slot, count):
        val = project(wbuf[pl.ds(2 * slot, 2 * count)].reshape(2 * count * pair, ch))
        for n in range(2 * count):
            keep(val, n % 2, slot + n // 2, n)

    def project_q(slot, count):
        val = project(wqbuf[pl.ds(slot, count)].reshape(count * pair, ch))
        for n in range(count):
            keep(val, 2, slot + n, n)

    def remote(src, dst, sem_s, sem_r, rr, cc, core):
        return pltpu.make_async_remote_copy(
            src_ref=src, dst_ref=dst, send_sem=sem_s, recv_sem=sem_r,
            device_id=(z, rr, cc, core), device_id_type=MESH)

    def kv_send(i, g):
        rr, cc = chip_to(i)
        for b in range(2):
            for n, dst in ((0, k_all), (1, v_all)):
                remote(sbuf.at[n, i + 1, b], dst.at[i + 1, k], send_sem.at[0], kv_sem.at[g], rr, cc, b).start()

    def q_send(i):
        rr, cc = chip_to(i, q_order)
        for b in range(2):
            remote(sbuf.at[2, i, b], q_all.at[i, k], send_sem.at[0], q_sem.at[i // UNIT], rr, cc, b).start()

    def kv_group(g, start, count):
        loaded(wbuf, 2 * (start + 1), 2 * count, w_sem.at[g])
        project_kv(start + 1, count)

    def kv_group_send(g, start, count):
        for n in range(count):
            kv_send(start + n, g)

    x_copy.wait()
    load_kv(2)
    kv_group(0, *groups[0])
    for g in range(3, n_group):
        load_kv(g)
    kv_group(1, *groups[1])
    with jax.named_scope("barrier"):
        pl.semaphore_wait(barrier, 2 * n_step + 1)
    kv_group_send(0, *groups[0])
    kv_group_send(1, *groups[1])

    def kv_loop(g, _):
        load_q(g - 2)
        start = (g - 2) * WIDE + groups[2][0]
        kv_group(g, start, WIDE)
        kv_group_send(g, start, WIDE)
        return 0

    with jax.named_scope("kv_loop"):
        lax.fori_loop(2, n_group, kv_loop, 0)

    for g in range(n_group - 2, n_q):
        load_q(g)
    kv_weights(own, my_chip, w_sem.at[n_group])
    q_weights(q_own, my_chip, w_sem.at[n_group])

    def q_loop(g, _):
        start = g * WIDE
        loaded(wqbuf, start, WIDE, wq_sem.at[g])
        project_q(start, WIDE)
        return 0

    with jax.named_scope("q_loop"):
        lax.fori_loop(0, n_q, q_loop, 0)

    def flip(slot):
        val = v_all[slot].reshape(2 * tok, pair)
        vt[:, slot * 2 * tok:(slot + 1) * 2 * tok] = val.T

    def kv_arrive(g):
        start, count = groups[g]
        part = sbuf.at[pl.ds(0, 2), pl.ds(start + 1, count)]
        pltpu.make_async_copy(part, part, kv_sem.at[g]).wait()
        for i in range(start, start + count):
            q_send(i)
        for i in range(start, start + count):
            flip(i + 1)

    kv_arrive(0)
    kv_arrive(1)

    with jax.named_scope("own"):
        for i in range(n_step):
            pltpu.make_async_copy(wo_hbm.at[chip_id(i, q_order)], wobuf.at[i], wo_sem).start()
        pltpu.make_async_copy(wo_hbm.at[my_chip], wobuf.at[q_own], wo_sem).start()
        loaded(wbuf, 2 * own, 2, w_sem.at[n_group])
        loaded(wqbuf, q_own, 1, w_sem.at[n_group])
        project_kv(own, 1)
        project_q(q_own, 1)
        for n, dst, at in ((0, k_all, own), (1, v_all, own), (2, q_all, q_own)):
            dst[at, k] = sbuf[n, at, k]
            remote(sbuf.at[n, at, 1 - k], dst.at[at, k], send_sem.at[1], kv_sem.at[n_group], r, c, 1 - k).start()

    with jax.named_scope("kv_arrive"):
        for g in range(2, n_group):
            kv_arrive(g)
        part = sbuf.at[:, 0, 0]
        pltpu.make_async_copy(part, part, kv_sem.at[n_group]).wait()
        flip(own)

    def arrived(ref, slot, count, sem):
        part = ref.at[pl.ds(slot, count)]
        pltpu.make_async_copy(part, part, sem).wait()

    keys = chips * 2 * tok
    lanes = 4 * tok * UNIT
    n_unit = chips // UNIT

    def queries(unit):
        parts = []
        for u in range(UNIT):
            q = q_all[unit * UNIT + u].reshape(2 * tok, pair) * BF16(head**-0.5)
            first = lax.broadcasted_iota(jnp.int32, q.shape, 1) < head
            zero = jnp.zeros_like(q)
            parts += [jnp.where(first, q, zero), jnp.where(first, zero, q)]
        return jnp.concatenate(parts, axis=0)

    def scores(qq, scr, lo, n):
        keys_c = k_all[lo // (2 * tok):(lo + n) // (2 * tok)].reshape(n, pair)
        s = lax.dot_general(keys_c, qq, NT, preferred_element_type=F32)
        scr[lo:lo + n] = s
        return jnp.max(s.reshape(n // 8, 8, lanes), axis=0)

    def weigh(scr, top, lo, n):
        w = jnp.exp(scr[lo:lo + n] - top)
        part = jnp.sum(w.reshape(n // 8, 8, lanes), axis=0)
        return part, lax.dot_general(vt[:, lo:lo + n], w.astype(BF16), NN, preferred_element_type=F32)

    def both(scr, top, next_unit, next_scr):
        new_top = total = acc = None
        qq = None if next_unit is None else queries(next_unit)
        for at in range(0, keys, KEY_CHUNK):
            if qq is not None:
                high = scores(qq, next_scr, at, KEY_CHUNK)
                new_top = high if new_top is None else jnp.maximum(new_top, high)
            if scr is not None:
                part, piece = weigh(scr, top, at, KEY_CHUNK)
                total = part if total is None else total + part
                acc = piece if acc is None else acc + piece
        if qq is not None:
            new_top = jnp.max(new_top, axis=0, keepdims=True)
        outs = []
        if scr is not None:
            total = jnp.sum(total, axis=0, keepdims=True)
            wide = 2 * tok
            for u in range(UNIT):
                a, b, e = 2 * u * wide, (2 * u + 1) * wide, (2 * u + 2) * wide
                out = jnp.concatenate([acc[:head, a:b] / total[:, a:b], acc[head:, b:e] / total[:, b:e]], axis=0)
                outs.append(out.T.astype(BF16))
        return outs, new_top

    half_slots = chips // 2

    def put(slot, out):
        rr, cc = chip_from(slot, q_order)
        for core in range(2):
            obuf[slot, core] = out[core * tok:(core + 1) * tok]
            remote(obuf.at[slot, core], ob.at[k, :, pl.ds(pl.multiple_of(slot * pair, pair), pair)],
                   send_sem.at[2], o_sem.at[slot // half_slots], rr, cc, core).start()

    def put_own(out):
        for core in range(2):
            obuf[q_own, core] = out[core * tok:(core + 1) * tok]
        at = pl.ds(q_own * pair, pair)
        ob[k, :, at] = obuf[q_own, k]
        remote(obuf.at[q_own, 1 - k], ob.at[k, :, at], send_sem.at[3], o_sem.at[2], r, c, 1 - k).start()

    def q_wait(unit, count=UNIT):
        with jax.named_scope("q_wait"):
            arrived(q_all, 0, count, q_sem.at[unit])

    def attend(j, top):
        unit = 2 * j
        for scr, next_scr in ((s0, s1), (s1, s0)):
            q_wait(unit + 1)
            outs, top = both(scr, top, unit + 1, next_scr)
            for u in range(UNIT):
                put(unit * UNIT + u, outs[u])
            unit = unit + 1
        return top

    q_wait(0)
    _, top = both(None, None, 0, s0)
    with jax.named_scope("attend"):
        top = lax.fori_loop(0, (n_unit - 2) // 2, attend, top)
    with jax.named_scope("last"):
        q_wait(n_unit - 1, UNIT - 1)
        outs, top = both(s0, top, n_unit - 1, s1)
        for u in range(UNIT):
            put((n_unit - 2) * UNIT + u, outs[u])
        outs, _ = both(s1, top, None, None)
        put(q_own - 1, outs[0])
        put_own(outs[1])

    blk = BLOCK
    cut = half_slots * pair

    def o_first(n, _):
        cs = pl.ds(pl.multiple_of(n * blk, blk), blk)
        lhs = ob[:, :, :cut].reshape(2 * tok, cut)
        w = wobuf[:half_slots, :, cs].reshape(cut, blk)
        y_part[:, cs] = lax.dot_general(lhs, w, NN, preferred_element_type=F32)
        return 0

    with jax.named_scope("o_arrive1"):
        pltpu.make_async_copy(wo_hbm, wobuf, wo_sem).wait()
        arrived(obuf, 0, half_slots, o_sem.at[0])
    with jax.named_scope("o_first"):
        lax.fori_loop(0, ch // blk, o_first, 0)
    with jax.named_scope("drain"):
        rest = sbuf.at[:, pl.ds(1, n_step)]
        pltpu.make_async_copy(rest, rest, send_sem.at[0]).wait()
        pltpu.make_async_copy(sbuf.at[:, 0, 0], sbuf.at[:, 0, 0], send_sem.at[1]).wait()
        pltpu.make_async_copy(obuf.at[0, 0], obuf.at[0, 0], send_sem.at[3]).wait()
        arrived(obuf, 0, n_step, send_sem.at[2])
    with jax.named_scope("o_arrive2"):
        arrived(obuf, half_slots, n_step - half_slots, o_sem.at[1])
        pltpu.make_async_copy(obuf.at[0, 0], obuf.at[0, 0], o_sem.at[2]).wait()


def finish_kernel(ob, wobuf, y_part, y_hbm, y_ref, y_sem):
    _, tok, width = ob.shape
    chips, pair, ch = wobuf.shape
    half, cut = chips // 2, width // 2

    def second(n, _):
        cs = pl.ds(pl.multiple_of(n * BLOCK, BLOCK), BLOCK)
        lhs = ob[:, :, cut:].reshape(2 * tok, width - cut)
        w = wobuf[half:, :, cs].reshape(width - cut, BLOCK)
        y = y_part[:, cs] + lax.dot_general(lhs, w, NN, preferred_element_type=F32)
        y_ref[:, cs] = y.astype(BF16)
        pltpu.make_async_copy(y_ref.at[:, cs], y_hbm.at[:, cs], y_sem).start()
        return 0

    lax.fori_loop(0, ch // BLOCK, second, 0)
    pltpu.make_async_copy(y_ref, y_hbm, y_sem).wait()


def solution(mesh):
    tok_spec = P("data", ("row", "col", "core"), None)
    rows, cols, cores = mesh.shape["row"], mesh.shape["col"], mesh.shape["core"]

    def per_device(tokens, w_qkv, w_out):
        batch, tok, ch = tokens.shape
        _, _, heads, head = w_qkv.shape
        chips = rows * cols
        pair = heads // chips * head
        dims = (rows, cols, tok, pair, head)
        keys = chips * cores * tok
        wt = jnp.transpose(w_qkv, (1, 2, 3, 0)).reshape(3 * chips, pair, ch)
        wo = w_out.reshape(chips, pair, ch)
        dma = pltpu.SemaphoreType.DMA
        n_group = len(groups_of(chips - 1))
        vmem = pl.BlockSpec(memory_space=pltpu.VMEM)
        ob, wobuf, y_part = pl.pallas_call(
            functools.partial(kernel, dims),
            out_shape=(
                pltpu.VMEM((2, tok, heads * head), BF16),
                pltpu.VMEM((chips, pair, ch), BF16),
                pltpu.VMEM((batch * tok, ch), F32),
            ),
            in_specs=[pl.BlockSpec(memory_space=pl.ANY)] * 3,
            out_specs=(vmem, vmem, vmem),
            scratch_shapes=[
                pltpu.VMEM((batch * tok, ch), BF16),
                pltpu.VMEM((2 * chips, pair, ch), BF16),
                pltpu.VMEM((chips, pair, ch), BF16),
                pltpu.VMEM((3, chips, 2, tok, pair), BF16),
                pltpu.VMEM((chips, 2, tok, pair), BF16),
                pltpu.VMEM((chips, 2, tok, pair), BF16),
                pltpu.VMEM((chips, 2, tok, pair), BF16),
                pltpu.VMEM((pair, keys), BF16),
                pltpu.VMEM((keys, 4 * tok * UNIT), F32),
                pltpu.VMEM((keys, 4 * tok * UNIT), F32),
                pltpu.VMEM((chips, 2, tok, pair), BF16),
                dma,
                dma((n_group + 1,)),
                dma(((chips - 1) // WIDE,)),
                dma,
                dma((4,)),
                dma((n_group + 1,)),
                dma((chips // 2,)),
                dma((3,)),
            ],
            compiler_params=pltpu.CompilerParams(
                collective_id=0, has_side_effects=True, vmem_limit_bytes=44 * 1024 * 1024),
        )(tokens.reshape(batch * tok, ch), wt, wo)
        y = pl.pallas_call(
            finish_kernel,
            out_shape=jax.ShapeDtypeStruct((batch * tok, ch), BF16),
            in_specs=[vmem] * 3,
            out_specs=pl.BlockSpec(memory_space=pl.ANY),
            scratch_shapes=[pltpu.VMEM((batch * tok, ch), BF16), dma],
            compiler_params=pltpu.CompilerParams(vmem_limit_bytes=8 * 1024 * 1024),
        )(ob, wobuf, y_part)
        return y.reshape(batch, tok, ch)

    return jax.shard_map(per_device, mesh=mesh, in_specs=(tok_spec, P(), P()), out_specs=tok_spec, check_vma=False)
```

```python
import functools

import jax
import jax.numpy as jnp
from jax import lax
from jax.experimental import pallas as pl
from jax.experimental.pallas import tpu as pltpu
from jax.sharding import PartitionSpec as P

MESH = pl.DeviceIdType.MESH
F32 = jnp.float32
BF16 = jnp.bfloat16
NT = (((1,), (1,)), ((), ()))
NN = (((1,), (0,)), ((), ()))
KEY_CHUNK = 512
WIDE = 3
UNIT = 2
BLOCK = 2048


def groups_of(n_step):
    sizes = [1, WIDE - 1] + [WIDE] * (n_step // WIDE - 1)
    starts = [sum(sizes[:g]) for g in range(len(sizes))]
    return list(zip(starts, sizes))


def hop_order(rows, cols):
    def hops(d, n):
        return min(d, n - d)

    offs = [(dy, dx) for dy in range(rows) for dx in range(cols)][1:]
    like = [[(2, 2)], [(1, 1), (3, 3)], [(2, 1), (2, 3), (0, 2)], [(1, 2), (3, 2), (2, 0)], [(1, 3), (3, 1), (0, 1)]]
    first = [o for group in like for o in group if o in offs]
    rest = [o for o in offs if o not in first]
    return first + sorted(rest, key=lambda o: -hops(o[0], rows) - hops(o[1], cols))


def query_order(rows, cols):
    def hops(d, n):
        return min(d, n - d)

    offs = [(dy, dx) for dy in range(rows) for dx in range(cols)][1:]
    near, mid, far = ([o for o in offs if lo <= hops(o[0], rows) + hops(o[1], cols) <= hi] for lo, hi in ((1, 1), (2, 2), (3, 4)))
    return near[:3] + mid + far + near[3:]


def pack_table(values, base):
    words = []
    for start in range(0, len(values), 8):
        words.append(sum(v * base**i for i, v in enumerate(values[start : start + 8])))
    return words


def kernel(dims, x_hbm, wt_hbm, wo_hbm, ob, wobuf, y_part, x_ref, wbuf, wqbuf, sbuf, k_all, v_all, q_all, vt, s0, s1, obuf,
           x_sem, w_sem, wq_sem, wo_sem, send_sem, kv_sem, q_sem, o_sem):
    rows, cols, tok, pair, head = dims
    chips = rows * cols
    ch = x_ref.shape[1]
    z = lax.axis_index("data")
    r = lax.axis_index("row")
    c = lax.axis_index("col")
    k = lax.axis_index("core")
    my_chip = r * cols + c
    order = hop_order(rows, cols)
    q_order = query_order(rows, cols)
    n_step = len(order)
    groups = groups_of(n_step)
    n_group = len(groups)
    own = 0
    q_own = n_step
    words = {id(o): (pack_table([d[0] for d in o], rows), pack_table([d[1] for d in o], cols)) for o in (order, q_order)}

    def digit(table, base, i):
        val = table[0]
        for w, word in enumerate(table[1:]):
            val = val + (word - table[w]) * (jnp.minimum(i // (8 * (w + 1)), 1))
        shift = base.bit_length() - 1
        return lax.rem(lax.shift_right_logical(jnp.int32(0) + val, shift * lax.rem(i, 8)), base)

    def offset(i, table):
        if isinstance(i, int):
            return table[i]
        dy_words, dx_words = words[id(table)]
        return digit(dy_words, rows, i), digit(dx_words, cols, i)

    def chip_to(i, table=order):
        dy, dx = offset(i, table)
        return lax.rem(r + dy, rows), lax.rem(c + dx, cols)

    def chip_from(i, table=order):
        dy, dx = offset(i, table)
        return lax.rem(r + rows - dy, rows), lax.rem(c + cols - dx, cols)

    x_copy = pltpu.make_async_copy(x_hbm, x_ref, x_sem)
    x_copy.start()

    def kv_weights(slot, chip, sem):
        for n in range(2):
            pltpu.make_async_copy(wt_hbm.at[(n + 1) * chips + chip], wbuf.at[2 * slot + n], sem).start()

    def q_weights(slot, chip, sem):
        pltpu.make_async_copy(wt_hbm.at[chip], wqbuf.at[slot], sem).start()

    def chip_id(i, table=order):
        rr, cc = chip_to(i, table)
        return rr * cols + cc

    n_q = n_step // WIDE

    def load_kv(g):
        start, count = groups[g]
        for i in range(start, start + count):
            kv_weights(i + 1, chip_id(i), w_sem.at[g])

    def load_q(g):
        for n in range(WIDE):
            i = g * WIDE + n
            q_weights(i, chip_id(i, q_order), wq_sem.at[g])

    def loaded(ref, slot, count, sem):
        part = ref.at[pl.ds(slot, count)]
        pltpu.make_async_copy(part, part, sem).wait()

    load_kv(0)
    barrier = pltpu.get_barrier_semaphore()
    for i in range(n_step):
        rr, cc = chip_to(i)
        for core in range(2):
            pl.semaphore_signal(barrier, inc=1, device_id=(z, rr, cc, core), device_id_type=MESH)
    pl.semaphore_signal(barrier, inc=1, device_id=(z, r, c, 1 - k), device_id_type=MESH)

    load_kv(1)

    def project(w):
        return lax.dot_general(w, x_ref[...], NT, preferred_element_type=F32).astype(BF16).T

    def keep(val, piece, slot, n):
        for b in range(2):
            sbuf[piece, slot, b] = val[b * tok:(b + 1) * tok, n * pair:(n + 1) * pair]

    def project_kv(slot, count):
        val = project(wbuf[pl.ds(2 * slot, 2 * count)].reshape(2 * count * pair, ch))
        for n in range(2 * count):
            keep(val, n % 2, slot + n // 2, n)

    def project_q(slot, count):
        val = project(wqbuf[pl.ds(slot, count)].reshape(count * pair, ch))
        for n in range(count):
            keep(val, 2, slot + n, n)

    def remote(src, dst, sem_s, sem_r, rr, cc, core):
        return pltpu.make_async_remote_copy(
            src_ref=src, dst_ref=dst, send_sem=sem_s, recv_sem=sem_r,
            device_id=(z, rr, cc, core), device_id_type=MESH)

    def kv_send(i, g):
        rr, cc = chip_to(i)
        for b in range(2):
            for n, dst in ((0, k_all), (1, v_all)):
                remote(sbuf.at[n, i + 1, b], dst.at[i + 1, k], send_sem.at[0], kv_sem.at[g], rr, cc, b).start()

    def q_send(i):
        rr, cc = chip_to(i, q_order)
        for b in range(2):
            remote(sbuf.at[2, i, b], q_all.at[i, k], send_sem.at[0], q_sem.at[i // UNIT], rr, cc, b).start()

    def kv_group(g, start, count):
        loaded(wbuf, 2 * (start + 1), 2 * count, w_sem.at[g])
        project_kv(start + 1, count)

    def kv_group_send(g, start, count):
        for n in range(count):
            kv_send(start + n, g)

    x_copy.wait()
    load_kv(2)
    kv_group(0, *groups[0])
    for g in range(3, n_group):
        load_kv(g)
    kv_group(1, *groups[1])
    with jax.named_scope("barrier"):
        pl.semaphore_wait(barrier, 2 * n_step + 1)
    kv_group_send(0, *groups[0])
    kv_group_send(1, *groups[1])

    def kv_loop(g, _):
        load_q(g - 2)
        start = (g - 2) * WIDE + groups[2][0]
        kv_group(g, start, WIDE)
        kv_group_send(g, start, WIDE)
        return 0

    with jax.named_scope("kv_loop"):
        lax.fori_loop(2, n_group, kv_loop, 0)

    for g in range(n_group - 2, n_q):
        load_q(g)
    kv_weights(own, my_chip, w_sem.at[n_group])
    q_weights(q_own, my_chip, w_sem.at[n_group])

    def q_loop(g, _):
        start = g * WIDE
        loaded(wqbuf, start, WIDE, wq_sem.at[g])
        project_q(start, WIDE)
        return 0

    with jax.named_scope("q_loop"):
        lax.fori_loop(0, n_q, q_loop, 0)

    def flip(slot):
        val = v_all[slot].reshape(2 * tok, pair)
        vt[:, slot * 2 * tok:(slot + 1) * 2 * tok] = val.T

    def kv_arrive(g):
        start, count = groups[g]
        part = sbuf.at[pl.ds(0, 2), pl.ds(start + 1, count)]
        pltpu.make_async_copy(part, part, kv_sem.at[g]).wait()
        for i in range(start, start + count):
            q_send(i)
        if g < n_group - 1:
            for i in range(start, start + count):
                flip(i + 1)

    kv_arrive(0)
    kv_arrive(1)

    with jax.named_scope("own"):
        for i in range(n_step):
            pltpu.make_async_copy(wo_hbm.at[chip_id(i, q_order)], wobuf.at[i], wo_sem).start()
        pltpu.make_async_copy(wo_hbm.at[my_chip], wobuf.at[q_own], wo_sem).start()
        loaded(wbuf, 2 * own, 2, w_sem.at[n_group])
        loaded(wqbuf, q_own, 1, w_sem.at[n_group])
        project_kv(own, 1)
        project_q(q_own, 1)
        for n, dst, at in ((0, k_all, own), (1, v_all, own), (2, q_all, q_own)):
            dst[at, k] = sbuf[n, at, k]
            remote(sbuf.at[n, at, 1 - k], dst.at[at, k], send_sem.at[1], kv_sem.at[n_group], r, c, 1 - k).start()

    with jax.named_scope("kv_arrive"):
        for g in range(2, n_group - 1):
            kv_arrive(g)
        part = sbuf.at[:, 0, 0]
        pltpu.make_async_copy(part, part, kv_sem.at[n_group]).wait()
        flip(own)
        kv_arrive(n_group - 1)

    def arrived(ref, slot, count, sem):
        part = ref.at[pl.ds(slot, count)]
        pltpu.make_async_copy(part, part, sem).wait()

    keys = chips * 2 * tok
    lanes = 4 * tok * UNIT
    n_unit = chips // UNIT

    def queries(unit):
        parts = []
        for u in range(UNIT):
            q = q_all[unit * UNIT + u].reshape(2 * tok, pair) * BF16(head**-0.5)
            first = lax.broadcasted_iota(jnp.int32, q.shape, 1) < head
            zero = jnp.zeros_like(q)
            parts += [jnp.where(first, q, zero), jnp.where(first, zero, q)]
        return jnp.concatenate(parts, axis=0)

    def scores(qq, scr, lo, n):
        keys_c = k_all[lo // (2 * tok):(lo + n) // (2 * tok)].reshape(n, pair)
        s = lax.dot_general(keys_c, qq, NT, preferred_element_type=F32)
        scr[lo:lo + n] = s
        return jnp.max(s.reshape(n // 8, 8, lanes), axis=0)

    def weigh(scr, top, lo, n):
        w = jnp.exp(scr[lo:lo + n] - top)
        part = jnp.sum(w.reshape(n // 8, 8, lanes), axis=0)
        return part, lax.dot_general(vt[:, lo:lo + n], w.astype(BF16), NN, preferred_element_type=F32)

    def both(scr, top, next_unit, next_scr):
        new_top = total = acc = None
        qq = None if next_unit is None else queries(next_unit)
        for at in range(0, keys, KEY_CHUNK):
            if qq is not None:
                high = scores(qq, next_scr, at, KEY_CHUNK)
                new_top = high if new_top is None else jnp.maximum(new_top, high)
            if scr is not None:
                part, piece = weigh(scr, top, at, KEY_CHUNK)
                total = part if total is None else total + part
                acc = piece if acc is None else acc + piece
        if qq is not None:
            new_top = jnp.max(new_top, axis=0, keepdims=True)
        outs = []
        if scr is not None:
            total = jnp.sum(total, axis=0, keepdims=True)
            wide = 2 * tok
            for u in range(UNIT):
                a, b, e = 2 * u * wide, (2 * u + 1) * wide, (2 * u + 2) * wide
                out = jnp.concatenate([acc[:head, a:b] / total[:, a:b], acc[head:, b:e] / total[:, b:e]], axis=0)
                outs.append(out.T.astype(BF16))
        return outs, new_top

    half_slots = chips // 2

    def put(slot, out):
        rr, cc = chip_from(slot, q_order)
        for core in range(2):
            obuf[slot, core] = out[core * tok:(core + 1) * tok]
            remote(obuf.at[slot, core], ob.at[k, :, pl.ds(pl.multiple_of(slot * pair, pair), pair)],
                   send_sem.at[2], o_sem.at[slot // half_slots], rr, cc, core).start()

    def put_own(out):
        for core in range(2):
            obuf[q_own, core] = out[core * tok:(core + 1) * tok]
        at = pl.ds(q_own * pair, pair)
        ob[k, :, at] = obuf[q_own, k]
        remote(obuf.at[q_own, 1 - k], ob.at[k, :, at], send_sem.at[3], o_sem.at[2], r, c, 1 - k).start()

    def q_wait(unit, count=UNIT):
        with jax.named_scope("q_wait"):
            arrived(q_all, 0, count, q_sem.at[unit])

    def attend(j, top):
        unit = 2 * j
        for scr, next_scr in ((s0, s1), (s1, s0)):
            q_wait(unit + 1)
            outs, top = both(scr, top, unit + 1, next_scr)
            for u in range(UNIT):
                put(unit * UNIT + u, outs[u])
            unit = unit + 1
        return top

    q_wait(0)
    _, top = both(None, None, 0, s0)
    for i in range(groups[-1][0], sum(groups[-1])):
        flip(i + 1)
    with jax.named_scope("attend"):
        top = lax.fori_loop(0, (n_unit - 2) // 2, attend, top)
    with jax.named_scope("last"):
        q_wait(n_unit - 1, UNIT - 1)
        outs, top = both(s0, top, n_unit - 1, s1)
        for u in range(UNIT):
            put((n_unit - 2) * UNIT + u, outs[u])
        outs, _ = both(s1, top, None, None)
        put(q_own - 1, outs[0])
        put_own(outs[1])

    blk = BLOCK
    cut = half_slots * pair

    def o_first(n, _):
        cs = pl.ds(pl.multiple_of(n * blk, blk), blk)
        lhs = ob[:, :, :cut].reshape(2 * tok, cut)
        w = wobuf[:half_slots, :, cs].reshape(cut, blk)
        y_part[:, cs] = lax.dot_general(lhs, w, NN, preferred_element_type=F32)
        return 0

    with jax.named_scope("o_arrive1"):
        pltpu.make_async_copy(wo_hbm, wobuf, wo_sem).wait()
        arrived(obuf, 0, half_slots, o_sem.at[0])
    with jax.named_scope("o_first"):
        lax.fori_loop(0, ch // blk, o_first, 0)
    with jax.named_scope("drain"):
        rest = sbuf.at[:, pl.ds(1, n_step)]
        pltpu.make_async_copy(rest, rest, send_sem.at[0]).wait()
        pltpu.make_async_copy(sbuf.at[:, 0, 0], sbuf.at[:, 0, 0], send_sem.at[1]).wait()
        pltpu.make_async_copy(obuf.at[0, 0], obuf.at[0, 0], send_sem.at[3]).wait()
        arrived(obuf, 0, n_step, send_sem.at[2])
    with jax.named_scope("o_arrive2"):
        arrived(obuf, half_slots, n_step - half_slots, o_sem.at[1])
        pltpu.make_async_copy(obuf.at[0, 0], obuf.at[0, 0], o_sem.at[2]).wait()


def finish_kernel(ob, wobuf, y_part, y_hbm, y_ref, y_sem):
    _, tok, width = ob.shape
    chips, pair, ch = wobuf.shape
    half, cut = chips // 2, width // 2

    def second(n, _):
        cs = pl.ds(pl.multiple_of(n * BLOCK, BLOCK), BLOCK)
        lhs = ob[:, :, cut:].reshape(2 * tok, width - cut)
        w = wobuf[half:, :, cs].reshape(width - cut, BLOCK)
        y = y_part[:, cs] + lax.dot_general(lhs, w, NN, preferred_element_type=F32)
        y_ref[:, cs] = y.astype(BF16)
        pltpu.make_async_copy(y_ref.at[:, cs], y_hbm.at[:, cs], y_sem).start()
        return 0

    lax.fori_loop(0, ch // BLOCK, second, 0)
    pltpu.make_async_copy(y_ref, y_hbm, y_sem).wait()


def solution(mesh):
    tok_spec = P("data", ("row", "col", "core"), None)
    rows, cols, cores = mesh.shape["row"], mesh.shape["col"], mesh.shape["core"]

    def per_device(tokens, w_qkv, w_out):
        batch, tok, ch = tokens.shape
        _, _, heads, head = w_qkv.shape
        chips = rows * cols
        pair = heads // chips * head
        dims = (rows, cols, tok, pair, head)
        keys = chips * cores * tok
        wt = jnp.transpose(w_qkv, (1, 2, 3, 0)).reshape(3 * chips, pair, ch)
        wo = w_out.reshape(chips, pair, ch)
        dma = pltpu.SemaphoreType.DMA
        n_group = len(groups_of(chips - 1))
        vmem = pl.BlockSpec(memory_space=pltpu.VMEM)
        ob, wobuf, y_part = pl.pallas_call(
            functools.partial(kernel, dims),
            out_shape=(
                pltpu.VMEM((2, tok, heads * head), BF16),
                pltpu.VMEM((chips, pair, ch), BF16),
                pltpu.VMEM((batch * tok, ch), F32),
            ),
            in_specs=[pl.BlockSpec(memory_space=pl.ANY)] * 3,
            out_specs=(vmem, vmem, vmem),
            scratch_shapes=[
                pltpu.VMEM((batch * tok, ch), BF16),
                pltpu.VMEM((2 * chips, pair, ch), BF16),
                pltpu.VMEM((chips, pair, ch), BF16),
                pltpu.VMEM((3, chips, 2, tok, pair), BF16),
                pltpu.VMEM((chips, 2, tok, pair), BF16),
                pltpu.VMEM((chips, 2, tok, pair), BF16),
                pltpu.VMEM((chips, 2, tok, pair), BF16),
                pltpu.VMEM((pair, keys), BF16),
                pltpu.VMEM((keys, 4 * tok * UNIT), F32),
                pltpu.VMEM((keys, 4 * tok * UNIT), F32),
                pltpu.VMEM((chips, 2, tok, pair), BF16),
                dma,
                dma((n_group + 1,)),
                dma(((chips - 1) // WIDE,)),
                dma,
                dma((4,)),
                dma((n_group + 1,)),
                dma((chips // 2,)),
                dma((3,)),
            ],
            compiler_params=pltpu.CompilerParams(
                collective_id=0, has_side_effects=True, vmem_limit_bytes=44 * 1024 * 1024),
        )(tokens.reshape(batch * tok, ch), wt, wo)
        y = pl.pallas_call(
            finish_kernel,
            out_shape=jax.ShapeDtypeStruct((batch * tok, ch), BF16),
            in_specs=[vmem] * 3,
            out_specs=pl.BlockSpec(memory_space=pl.ANY),
            scratch_shapes=[pltpu.VMEM((batch * tok, ch), BF16), dma],
            compiler_params=pltpu.CompilerParams(vmem_limit_bytes=8 * 1024 * 1024),
        )(ob, wobuf, y_part)
        return y.reshape(batch, tok, ch)

    return jax.shard_map(per_device, mesh=mesh, in_specs=(tok_spec, P(), P()), out_specs=tok_spec, check_vma=False)
```
